32 devices in a mesh: rows: 8 (over z, x), cols: 4 (over y, core).
Axes of the slice: x: 2, y: 2, z: 4, core: 2. Of those that a mesh axis runs over, the one named last changes fastest.
Arguments:
- vectors: bfloat16 [1024, 32768], P(None, 'rows'), may hold values from -0.4 to 0.4
- integrals: bfloat16 [2, 256, 32768], P(None, 'cols', 'rows'), may hold values from -8 to 72
- pivots: int32 [2, 256], replicated, may hold values from 0 to 32767, as said below
Outputs:
- new_vectors: float32 [2, 256, 32768], P(None, 'cols', 'rows')
The draws below stay inside these ranges and needn't reach their ends.
Inputs may be any that keep to these rules, and one draw needn't show every extreme that they name: The 2 x 256 entries are distinct shell-pair rows. In each panel the rows of one index of rows (an aligned block of 4096) hold at most 64 pivots, and some block holds exactly 64.
All inputs are finite; a program needn't handle non-finite values.
Results may differ from the reference program's by a relative error of at most 0.00036.
Values may be sent and summed in bfloat16 or wider, within the bound.
No kernel may reach another device: no remote copies, remote signals or barrier semaphores. Data moves between devices by JAX's collectives and lax.ppermute only.
A program may use at most 64 MiB of HBM per device.

```python
import jax
import jax.numpy as jnp

PRIOR = 1024
PW = 256
PANELS = 2
PAIR_DEV = 4096
PAIRS = 32768


group_width = 16


def pivot_lists(key):
    owners = PAIRS // PAIR_DEV
    slot_count = 2 * PW // owners
    half_count = slot_count // 2
    base = jax.random.fold_in(key, 7)
    ceiling = (2 ** 31 - 1) // PAIR_DEV - 1
    scores = jax.random.randint(jax.random.fold_in(base, 1), (owners, PAIR_DEV), 0, ceiling) * PAIR_DEV
    scores = scores + jnp.arange(PAIR_DEV, dtype=jnp.int32)[None, :]
    local_order = jnp.argsort(scores, axis=1, stable=True).astype(jnp.int32)
    offsets = jnp.zeros((owners,), jnp.int32)
    panels_out = []
    for panel in range(PANELS):
        panel_key = jax.random.fold_in(base, 100 + panel)
        swing = jax.random.randint(jax.random.fold_in(panel_key, 1), (owners // 2,), 0, half_count + 1)
        swing = swing.at[0].set(half_count)
        paired = jnp.stack([half_count + swing, half_count - swing], axis=1).reshape(-1)
        owner_scores = jax.random.randint(jax.random.fold_in(panel_key, 2), (owners,), 0, 2 ** 20) * owners
        owner_scores = owner_scores + jnp.arange(owners, dtype=jnp.int32)
        owner_order = jnp.argsort(owner_scores, stable=True).astype(jnp.int32)
        counts = jnp.zeros((owners,), jnp.int32).at[owner_order].set(paired.astype(jnp.int32))
        slots = jnp.arange(slot_count, dtype=jnp.int32)
        valid = slots[None, :] < counts[:, None]
        where = jnp.minimum(offsets[:, None] + slots[None, :], PAIR_DEV - 1)
        local_rows = jnp.take_along_axis(local_order, where, axis=1)
        global_rows = jnp.arange(owners, dtype=jnp.int32)[:, None] * PAIR_DEV + local_rows
        flat_rows = global_rows.reshape(-1)
        flat_invalid = (1 - valid.astype(jnp.int32)).reshape(-1)
        first = jnp.argsort(flat_invalid, stable=True)[:PW]
        chosen = flat_rows[first]
        shuffle_scores = jax.random.randint(jax.random.fold_in(panel_key, 3), (PW,), 0, 2 ** 20) * PW
        shuffle_scores = shuffle_scores + jnp.arange(PW, dtype=jnp.int32)
        shuffle = jnp.argsort(shuffle_scores, stable=True)
        panels_out.append(chosen[shuffle].astype(jnp.int32))
        offsets = offsets + counts
    return jnp.stack(panels_out)


def draw_pivots(key, part):
    return pivot_lists(key)


def draw_vectors(key, part):
    base_key = jax.random.fold_in(key, 21)
    factor = 2.0 * PRIOR ** (-0.5)
    values = jnp.clip(jax.random.normal(jax.random.fold_in(base_key, 5), (PRIOR, PAIRS), jnp.float32), -6.0, 6.0)
    return jnp.clip(values * factor, -0.3984375, 0.3984375).astype(jnp.bfloat16)


def draw_integrals(key, part):
    pivot_table = pivot_lists(key)
    noise_key = jax.random.fold_in(key, 11)
    noise = jnp.clip(jax.random.normal(noise_key, (PANELS, PW, PAIRS), jnp.float32), -6.0, 6.0)
    group_count = (PW + group_width - 1) // group_width
    strength = jax.random.uniform(jax.random.fold_in(key, 13), (PANELS, group_count), jnp.float32, 24.0, 40.0)
    position = jnp.arange(PW, dtype=jnp.int32)
    member = position // group_width
    same_group = (member[:, None] == member[None, :]).astype(jnp.float32)
    identity = (position[:, None] == position[None, :]).astype(jnp.float32)
    coupling = jnp.take(strength, member, axis=1)[:, :, None] * (same_group * (1.0 - identity))[None, :, :]
    pattern = 64.0 * identity[None, :, :] + coupling
    panel_index = jnp.arange(PANELS, dtype=jnp.int32)[:, None, None]
    row_index = position[None, :, None]
    column_index = pivot_table[:, None, :]
    structure = jnp.zeros((PANELS, PW, PAIRS), jnp.float32).at[panel_index, row_index, column_index].set(pattern)
    column_scale = jnp.ones((PAIRS,), jnp.float32).at[pivot_table.reshape(-1)].set(0.125)
    return (noise * column_scale[None, None, :] + structure).astype(jnp.bfloat16)


def setup_inputs(seed: int = 0) -> dict:
    streams_of = jax.random.split(jax.random.key(seed), 4)
    return {
        "vectors": draw_vectors(jax.random.fold_in(streams_of[3], 71), 0),
        "integrals": draw_integrals(jax.random.fold_in(streams_of[3], 71), 0),
        "pivots": draw_pivots(jax.random.fold_in(streams_of[3], 71), 0),
    }


def factor_panel(residual, pivot_row):
    block = jnp.take(residual, pivot_row, axis=1)
    symmetric = 0.5 * (block + block.T)
    lower_factor = jnp.linalg.cholesky(symmetric)
    return jax.scipy.linalg.solve_triangular(lower_factor, residual, lower=True)

def reference(vectors, integrals, pivots):
    factors = [vectors]
    results = []
    for panel in range(PANELS):
        pivot_row = pivots[panel].astype(jnp.int32)
        residual = integrals[panel].astype(jnp.float32)
        for factor in factors:
            chosen = jnp.take(factor, pivot_row, axis=1).T
            residual = residual - jnp.dot(chosen.astype(jnp.float32), factor.astype(jnp.float32), preferred_element_type=jnp.float32)
        fresh = factor_panel(residual, pivot_row)
        results.append(fresh)
        factors.append(fresh.astype(jnp.bfloat16))
    return jnp.stack(results)
```

```python
import functools

import jax
import jax.numpy as jnp
from jax import lax
from jax.experimental import pallas as pl
from jax.experimental.pallas import tpu as pltpu
from jax.sharding import PartitionSpec as P

LANES = 128
LEAF = 32
SUB = 16
CHUNK = 512
MIB = 1 << 20


def masks_of(size):
    return [1 << bit for bit in reversed(range(size.bit_length() - 1))]


def dot(left, right, left_dim=1, right_dim=0):
    return lax.dot_general(
        left, right, (((left_dim,), (right_dim,)), ((), ())), preferred_element_type=jnp.float32
    )


def split(x):
    high = x.astype(jnp.bfloat16)
    return high, (x - high.astype(jnp.float32)).astype(jnp.bfloat16)


def product_narrow(left, right, right_dim=0):
    rows = left.shape[0]
    both = dot(jnp.concatenate(split(left), 0), right, 1, right_dim)
    return both[:rows] + both[rows:]


def product_wide(left, right):
    left_high, left_low = split(left)
    right_high, right_low = split(right)
    return dot(
        jnp.concatenate([left_high, left_low, left_high], 1),
        jnp.concatenate([right_high, right_high, right_low], 0),
    )


def iota(shape, dim):
    return lax.broadcasted_iota(jnp.int32, shape, dim)


def as_column(row):
    size = row.shape[1]
    square = (size, size)
    return jnp.sum(
        jnp.where(iota(square, 0) == iota(square, 1), jnp.broadcast_to(row, square), 0.0),
        axis=1,
        keepdims=True,
    )


def select_kernel(slot_count, pivots_ref, vectors_ref, integrals_ref, out_ref, vec, ints, sems):
    part, row_count = vec.shape
    panels, block_cols, _ = ints.shape
    width = pivots_ref.shape[1]
    lanes = panels * slot_count
    first = lax.axis_index("cols") * part
    copies = [
        pltpu.make_async_copy(
            vectors_ref.at[pl.ds(pl.multiple_of(first, part), part), :], vec, sems.at[0]
        ),
        pltpu.make_async_copy(integrals_ref, ints, sems.at[1]),
    ]
    for copy in copies:
        copy.start()
    start = (lax.axis_index("rows") * row_count).astype(jnp.float32)
    square = (width, width)
    target = jnp.zeros((1, lanes), jnp.float32)
    for panel in range(panels):
        local = pivots_ref[panel : panel + 1, :].astype(jnp.float32) - start
        mine = ((local >= 0.0) & (local < row_count)).astype(jnp.float32)
        earlier = iota(square, 1) < iota(square, 0)
        rank = jnp.sum(
            jnp.where(earlier, jnp.broadcast_to(mine, square), 0.0), axis=1, keepdims=True
        )
        held = as_column(jnp.where(mine > 0.0, local + 1.0, 0.0))
        slot = iota((width, lanes), 1).astype(jnp.float32) - panel * slot_count
        target = target + jnp.sum(jnp.where(rank == slot, held, 0.0), axis=0, keepdims=True)
    target = target.astype(jnp.int32) - 1
    for copy in copies:
        copy.wait()
    step = min(CHUNK, row_count)
    found = jnp.zeros(out_ref.shape, jnp.float32)
    for offset in range(0, row_count, step):
        pick = jnp.where(iota((step, lanes), 0) + offset == target, 1.0, 0.0).astype(jnp.bfloat16)
        left = jnp.concatenate(
            [vec[:, offset : offset + step]]
            + [ints[panel, :, offset : offset + step] for panel in range(panels)],
            0,
        )
        found = found + dot(left, pick)
    out_ref[...] = found.astype(jnp.bfloat16)


def select(pivots, vectors, integrals, slot_count, part):
    panels, block_cols, row_count = integrals.shape
    rows = part + panels * block_cols
    lanes = panels * slot_count
    return pl.pallas_call(
        functools.partial(select_kernel, slot_count),
        out_shape=jax.ShapeDtypeStruct((rows, lanes), jnp.bfloat16),
        in_specs=[
            pl.BlockSpec(memory_space=pltpu.VMEM),
            pl.BlockSpec(memory_space=pl.ANY),
            pl.BlockSpec(memory_space=pl.ANY),
        ],
        out_specs=pl.BlockSpec(memory_space=pltpu.VMEM),
        scratch_shapes=[
            pltpu.VMEM((part, row_count), jnp.bfloat16),
            pltpu.VMEM(integrals.shape, jnp.bfloat16),
            pltpu.SemaphoreType.DMA((2,)),
        ],
        compiler_params=pltpu.CompilerParams(vmem_limit_bytes=16 * MIB),
        cost_estimate=pl.CostEstimate(
            flops=2 * rows * row_count * lanes, bytes_accessed=3 * MIB, transcendentals=0
        ),
        name="select",
    )(pivots, vectors, integrals)


def compact_kernel(masks, slot_count, row_count, pivots_ref, near_ref, far_ref, out_ref):
    panels, width = pivots_ref.shape
    half, rows, lanes = near_ref.shape
    shift = row_count.bit_length() - 1
    me = lax.axis_index("rows")
    square = (width, width)
    places = []
    for panel in range(panels):
        owner = lax.shift_right_logical(
            pivots_ref[panel : panel + 1, :], jnp.full((1, width), shift, jnp.int32)
        )
        floats = owner.astype(jnp.float32)
        same = jnp.broadcast_to(floats, square) == as_column(floats)
        earlier = iota(square, 0) < iota(square, 1)
        rank = jnp.sum(
            jnp.where(same & earlier, 1.0, 0.0), axis=0, keepdims=True
        ).astype(jnp.int32)
        apart = owner ^ me
        block = jnp.zeros_like(owner)
        for bit, mask in enumerate(masks):
            block = block + jnp.where((apart & mask) != 0, 1 << bit, 0)
        places.append(block * lanes + panel * slot_count + rank)
    place = jnp.concatenate(places, 1)
    total = jnp.zeros((rows, panels * width), jnp.float32)
    for block in range(2 * half):
        ref = near_ref if block < half else far_ref
        pick = jnp.where(
            iota((lanes, panels * width), 0) + block * lanes == place, 1.0, 0.0
        ).astype(jnp.bfloat16)
        total = total + dot(ref[block % half], pick)
    out_ref[...] = total.astype(jnp.bfloat16)


def compact(pivots, near, far, masks, slot_count, row_count):
    half, rows, lanes = near.shape
    width = pivots.shape[0] * pivots.shape[1]
    return pl.pallas_call(
        functools.partial(compact_kernel, masks, slot_count, row_count),
        out_shape=jax.ShapeDtypeStruct((rows, width), jnp.bfloat16),
        in_specs=[pl.BlockSpec(memory_space=pltpu.VMEM)] * 3,
        out_specs=pl.BlockSpec(memory_space=pltpu.VMEM),
        compiler_params=pltpu.CompilerParams(vmem_limit_bytes=16 * MIB),
        cost_estimate=pl.CostEstimate(
            flops=4 * half * rows * lanes * width, bytes_accessed=2 * MIB, transcendentals=0
        ),
        name="compact",
    )(pivots, near, far)


def eliminate(work, start, width):
    groups = 2 * width // LANES
    vregs = LEAF // 8
    rows = [
        [work[pl.ds(start + 8 * v, 8), LANES * g : LANES * (g + 1)] for v in range(vregs)]
        for g in range(groups)
    ]
    lane_group = start // LANES
    turn = lax.rem(LANES - lax.rem(start, LANES), LANES)
    sublane = iota((8, LANES), 0)
    pivots = [jnp.zeros((8, LANES), jnp.float32) for _ in range(vregs)]
    for sub in range(0, LEAF, SUB):
        first = sub // 8
        diagonal = []
        for v in range(first, vregs):
            picked = rows[0][v]
            for g in range(1, width // LANES):
                picked = jnp.where(lane_group == g, rows[g][v], picked)
            diagonal.append(pltpu.roll(picked, turn, 1))
        cols = [
            [jnp.broadcast_to(x[:, sub + k : sub + k + 1], (8, LANES)) for x in diagonal]
            for k in range(SUB)
        ]
        for j in range(SUB):
            jv, jr = j // 8, j % 8
            live = range(jv, len(diagonal))
            pivot = jnp.broadcast_to(cols[j][jv][jr : jr + 1, :], (8, LANES))
            inverse = 1.0 / pivot
            factor = {v: cols[j][v] * inverse for v in live}
            factor[jv] = jnp.where(sublane > jr, factor[jv], 0.0)
            pivots[first + jv] = jnp.where(sublane == jr, pivot, pivots[first + jv])
            for k in range(j + 1, SUB):
                entry = jnp.broadcast_to(cols[k][jv][jr : jr + 1, :], (8, LANES))
                for v in live:
                    cols[k][v] = cols[k][v] - factor[v] * entry
            for g in range(groups):
                entry = jnp.broadcast_to(rows[g][first + jv][jr : jr + 1, :], (8, LANES))
                for v in live:
                    rows[g][first + v] = rows[g][first + v] - factor[v] * entry
    scale = [lax.rsqrt(pivot) for pivot in pivots]
    return jnp.concatenate(
        [jnp.concatenate([x * s for x, s in zip(rows[g], scale)], 0) for g in range(groups)], 1
    )


def invert_factor(matrix, work, width):
    square = (width, width)
    work[:, :width] = 0.5 * (matrix + matrix.T)
    work[:, width:] = jnp.where(iota(square, 0) == iota(square, 1), 1.0, 0.0)

    def body(leaf, carry):
        start = pl.multiple_of(leaf * LEAF, LEAF)
        upper = eliminate(work, start, width)
        high, low = split(upper)
        later = iota((3 * LEAF, width), 1) >= start + LEAF
        left = jnp.concatenate([high[:, :width], low[:, :width], high[:, :width]], 0)
        left = jnp.where(later, left, jnp.zeros_like(left))
        work[...] = work[...] - dot(left, jnp.concatenate([high, high, low], 0), 0, 0)
        work[pl.ds(start, LEAF), :] = upper
        return carry

    lax.fori_loop(0, width // LEAF, body, 0)


def factor_kernel(apart, part, *refs):
    count = len(apart)
    picked = refs[:count]
    blocks = refs[count : 2 * count]
    vectors_ref, out_ref = refs[2 * count], refs[2 * count + 1]
    right, rows_of, ints0, ints1, work0, work1, left, result, sems, out_sems = refs[2 * count + 2 :]
    me = lax.axis_index("cols")
    prior, pairs = vectors_ref.shape
    panels, block_cols, _ = blocks[0].shape
    width = work0.shape[0]
    both = panels * width
    copies = [pltpu.make_async_copy(vectors_ref, right.at[both:, :], sems.at[0])]
    for i, bits in enumerate(apart):
        for panel in range(panels):
            at = pl.multiple_of(panel * width + (me ^ bits) * block_cols, block_cols)
            copies.append(
                pltpu.make_async_copy(
                    blocks[i].at[panel],
                    right.at[pl.ds(at, block_cols), :],
                    sems.at[1 + i * panels + panel],
                )
            )
    for copy in copies:
        copy.start()

    for i, bits in enumerate(apart):
        rows_of[pl.ds(pl.multiple_of((me ^ bits) * part, part), part), :] = picked[i][:part, :]
        at = pl.ds(pl.multiple_of((me ^ bits) * block_cols, block_cols), block_cols)
        ints0[at, :] = picked[i][part : part + block_cols, :].astype(jnp.float32)
        ints1[at, :] = picked[i][part + block_cols :, width:].astype(jnp.float32)
    at_pivots = rows_of[...]
    gram = dot(at_pivots, at_pivots, 0, 0)
    residual0 = ints0[...] - gram[:width, :]
    invert_factor(residual0[:, :width], work0, width)
    ahead = product_wide(work0[:, width:], residual0[:, width:]).astype(jnp.bfloat16)
    invert_factor(ints1[...] - gram[width:, width:] - dot(ahead, ahead, 0, 0), work1, width)

    mine = pl.ds(pl.multiple_of(me * block_cols, block_cols), block_cols)
    inverse0 = work0[mine, width:]
    inverse1 = work1[mine, width:]
    through = product_wide(product_narrow(inverse1, ahead, 1), work0[:, width:])
    on_vectors = product_narrow(
        jnp.concatenate(
            [
                jnp.concatenate([inverse0, jnp.zeros_like(inverse0)], 1),
                jnp.concatenate([-through, inverse1], 1),
            ],
            0,
        ),
        rows_of[...],
        1,
    )
    top = jnp.concatenate([inverse0, jnp.zeros_like(inverse0), -on_vectors[:block_cols]], 1)
    low = jnp.concatenate([-through, inverse1, -on_vectors[block_cols:]], 1)
    left[...] = jnp.concatenate(split(jnp.concatenate([top, low], 0)), 0)

    for copy in copies:
        copy.wait()
    outs = []
    for n in range(pairs // CHUNK):
        at = pl.ds(n * CHUNK, CHUNK)
        halves = dot(left[...], right[:, at])
        value = halves[: panels * block_cols] + halves[panels * block_cols :]
        for panel in range(panels):
            result[panel, :, at] = value[panel * block_cols : (panel + 1) * block_cols]
        outs.append(
            pltpu.make_async_copy(result.at[:, :, at], out_ref.at[:, :, at], out_sems.at[n])
        )
        outs[-1].start()
    for copy in outs:
        copy.wait()


def factor(picked, blocks, vectors, apart, part):
    panels, block_cols, pairs = blocks[0].shape
    prior = vectors.shape[0]
    both = picked[0].shape[1]
    width = both // panels
    count = len(apart)
    return pl.pallas_call(
        functools.partial(factor_kernel, apart, part),
        out_shape=jax.ShapeDtypeStruct((panels, block_cols, pairs), jnp.float32),
        in_specs=[pl.BlockSpec(memory_space=pltpu.VMEM)] * count
        + [pl.BlockSpec(memory_space=pl.ANY)] * (count + 1),
        out_specs=pl.BlockSpec(memory_space=pl.ANY),
        scratch_shapes=[
            pltpu.VMEM((both + prior, pairs), jnp.bfloat16),
            pltpu.VMEM((prior, both), jnp.bfloat16),
            pltpu.VMEM((width, both), jnp.float32),
            pltpu.VMEM((width, width), jnp.float32),
            pltpu.VMEM((width, 2 * width), jnp.float32),
            pltpu.VMEM((width, 2 * width), jnp.float32),
            pltpu.VMEM((2 * panels * block_cols, both + prior), jnp.bfloat16),
            pltpu.VMEM((panels, block_cols, pairs), jnp.float32),
            pltpu.SemaphoreType.DMA((1 + count * panels,)),
            pltpu.SemaphoreType.DMA((pairs // CHUNK,)),
        ],
        compiler_params=pltpu.CompilerParams(vmem_limit_bytes=40 * MIB),
        cost_estimate=pl.CostEstimate(
            flops=8 * panels * block_cols * (both + prior) * pairs,
            bytes_accessed=16 * MIB,
            transcendentals=0,
        ),
        name="factor",
    )(*picked, *blocks, vectors)


def per_device(vectors, integrals, pivots):
    prior, row_count = vectors.shape
    panels, width = pivots.shape
    owners, col_count = lax.axis_size("rows"), lax.axis_size("cols")
    slot_count = 2 * width // owners
    part = prior // col_count

    def swap(x, axis, size, mask):
        return lax.ppermute(x, axis, [(i, i ^ mask) for i in range(size)])

    def spread(x):
        pieces, apart = [x], [0]
        for mask in masks_of(col_count):
            pieces = pieces + [swap(piece, "cols", col_count, mask) for piece in pieces]
            apart = apart + [bits ^ mask for bits in apart]
        return pieces, apart

    found = select(pivots, vectors, integrals, slot_count, part)[None]
    masks = masks_of(owners)
    for mask in masks[:-1]:
        found = jnp.concatenate([found, swap(found, "rows", owners, mask)], 0)
    other = swap(found, "rows", owners, masks[-1])
    ordered = compact(pivots, found, other, masks, slot_count, row_count)
    picked, apart = spread(ordered)
    blocks, _ = spread(integrals)
    return factor(picked, blocks, vectors, apart, part)


def solution(mesh):
    placed = (P(None, "rows"), P(None, "cols", "rows"), P())
    return jax.shard_map(
        per_device, mesh=mesh, in_specs=placed, out_specs=P(None, "cols", "rows"), check_vma=False
    )
```

```python
import functools

import jax
import jax.numpy as jnp
from jax import lax
from jax.experimental import pallas as pl
from jax.experimental.pallas import tpu as pltpu
from jax.sharding import PartitionSpec as P

LANES = 128
LEAF = 32
SUB = 16
CHUNK = 512
SELECT = 1024
MICRO = 1 << 29
MIB = 1 << 20
ALMOST_ALL = 63 * MIB


def masks_of(size):
    return [1 << bit for bit in reversed(range(size.bit_length() - 1))]


def dot(left, right, left_dim=1, right_dim=0):
    return lax.dot_general(
        left, right, (((left_dim,), (right_dim,)), ((), ())), preferred_element_type=jnp.float32
    )


def split(x):
    high = x.astype(jnp.bfloat16)
    return high, (x - high.astype(jnp.float32)).astype(jnp.bfloat16)


def product_narrow(left, right, right_dim=0):
    rows = left.shape[0]
    both = dot(jnp.concatenate(split(left), 0), right, 1, right_dim)
    return both[:rows] + both[rows:]


def product_wide(left, right):
    left_high, left_low = split(left)
    right_high, right_low = split(right)
    return dot(
        jnp.concatenate([left_high, left_low, left_high], 1),
        jnp.concatenate([right_high, right_high, right_low], 0),
    )


def iota(shape, dim):
    return lax.broadcasted_iota(jnp.int32, shape, dim)


def as_column(row):
    size = row.shape[1]
    square = (size, size)
    return jnp.sum(
        jnp.where(iota(square, 0) == iota(square, 1), jnp.broadcast_to(row, square), 0.0),
        axis=1,
        keepdims=True,
    )


def pack(x):
    half = x.shape[0] // 2
    return jnp.concatenate([x[:half], x[half:]], 1)


def select_kernel(slot_count, pivots_ref, vectors_ref, integrals_ref, *refs):
    panels, block_cols, _ = integrals_ref.shape
    found_ref, out_refs = refs[0], refs[1 : 1 + panels]
    vec, ints, sems = refs[1 + panels :]
    part, row_count = vec.shape
    width = pivots_ref.shape[1]
    lanes = panels * slot_count
    first = pl.multiple_of(lax.axis_index("cols") * part, part)
    step = min(SELECT, row_count)
    count = row_count // step
    copies = []
    for n in range(count):
        at = pl.ds(n * step, step)
        copies.append(
            pltpu.make_async_copy(
                vectors_ref.at[pl.ds(first, part), at], vec.at[:, at], sems.at[n]
            )
        )
    whole = pltpu.make_async_copy(integrals_ref, ints, sems.at[count])
    for copy in copies[:1] + [whole] + copies[1:]:
        copy.start()
    start = (lax.axis_index("rows") * row_count).astype(jnp.float32)
    square = (width, width)
    target = jnp.zeros((1, lanes), jnp.float32)
    for panel in range(panels):
        local = pivots_ref[panel : panel + 1, :].astype(jnp.float32) - start
        mine = ((local >= 0.0) & (local < row_count)).astype(jnp.float32)
        earlier = iota(square, 1) < iota(square, 0)
        rank = jnp.sum(
            jnp.where(earlier, jnp.broadcast_to(mine, square), 0.0), axis=1, keepdims=True
        )
        held = as_column(jnp.where(mine > 0.0, local + 1.0, 0.0))
        slot = iota((width, lanes), 1).astype(jnp.float32) - panel * slot_count
        target = target + jnp.sum(jnp.where(rank == slot, held, 0.0), axis=0, keepdims=True)
    target = target.astype(jnp.int32) - 1
    whole.wait()
    outs = [
        pltpu.make_async_copy(ints.at[panel], out_refs[panel], sems.at[count + 1 + panel])
        for panel in range(panels)
    ]
    for copy in outs:
        copy.start()
    found = jnp.zeros((part + panels * block_cols, lanes), jnp.float32)
    for n, copy in enumerate(copies):
        copy.wait()
        at = slice(n * step, (n + 1) * step)
        pick = jnp.where(iota((step, lanes), 0) + n * step == target, 1.0, 0.0).astype(jnp.bfloat16)
        left = jnp.concatenate([vec[:, at]] + [ints[panel, :, at] for panel in range(panels)], 0)
        found = found + dot(left, pick)
    common = part + block_cols
    found_ref[:common, :] = found[:common].astype(jnp.bfloat16)
    found_ref[common:, :] = pack(found[common:, slot_count:]).astype(jnp.bfloat16)
    for copy in outs:
        copy.wait()


def select(pivots, vectors, integrals, slot_count, part):
    panels, block_cols, row_count = integrals.shape
    rows = part + block_cols + block_cols // 2
    outs = [jax.ShapeDtypeStruct((rows, panels * slot_count), jnp.bfloat16)]
    outs += [jax.ShapeDtypeStruct((block_cols, row_count), jnp.bfloat16)] * panels
    results = pl.pallas_call(
        functools.partial(select_kernel, slot_count),
        out_shape=outs,
        in_specs=[
            pl.BlockSpec(memory_space=pltpu.VMEM),
            pl.BlockSpec(memory_space=pltpu.HBM),
            pl.BlockSpec(memory_space=pltpu.HBM),
        ],
        out_specs=[pl.BlockSpec(memory_space=pltpu.VMEM)]
        + [pl.BlockSpec(memory_space=pltpu.HBM)] * panels,
        scratch_shapes=[
            pltpu.VMEM((part, row_count), jnp.bfloat16),
            pltpu.VMEM(integrals.shape, jnp.bfloat16),
            pltpu.SemaphoreType.DMA((row_count // min(SELECT, row_count) + 1 + panels,)),
        ],
        compiler_params=pltpu.CompilerParams(vmem_limit_bytes=ALMOST_ALL),
        cost_estimate=pl.CostEstimate(flops=MICRO * 2, bytes_accessed=3 * MIB, transcendentals=0),
        name="select",
    )(pivots, vectors, integrals)
    return results[0], results[1:]


def compact_kernel(weights, slot_count, row_count, pivots_ref, *refs):
    pieces, outs = refs[:-2], refs[-2:]
    panels, width = pivots_ref.shape
    depth, rows, lanes = pieces[0].shape
    common = outs[0].shape[0]
    shift = row_count.bit_length() - 1
    me = lax.axis_index("rows")
    square = (width, width)
    places = []
    for panel in range(panels):
        owner = lax.shift_right_logical(
            pivots_ref[panel : panel + 1, :], jnp.full((1, width), shift, jnp.int32)
        )
        floats = owner.astype(jnp.float32)
        same = jnp.broadcast_to(floats, square) == as_column(floats)
        earlier = iota(square, 0) < iota(square, 1)
        rank = jnp.sum(
            jnp.where(same & earlier, 1.0, 0.0), axis=0, keepdims=True
        ).astype(jnp.int32)
        apart = owner ^ me
        block = jnp.zeros_like(owner)
        for mask, weight in weights:
            block = block + jnp.where((apart & mask) != 0, weight, 0)
        places.append(block * lanes + rank)
    both = jnp.concatenate([places[0], places[1] + slot_count], 1)
    halves = jnp.concatenate([places[1], places[1] + slot_count], 1)
    main = jnp.zeros((common, 2 * width), jnp.float32)
    rest = jnp.zeros((rows - common, 2 * width), jnp.float32)
    for i in range(len(pieces) * depth):
        lane = iota((lanes, 2 * width), 0) + i * lanes
        x = pieces[i // depth][i % depth]
        main = main + dot(x[:common], jnp.where(lane == both, 1.0, 0.0).astype(jnp.bfloat16))
        rest = rest + dot(x[common:], jnp.where(lane == halves, 1.0, 0.0).astype(jnp.bfloat16))
    outs[0][...] = main[:, :width].astype(jnp.bfloat16)
    outs[1][:common, :] = main[:, width:].astype(jnp.bfloat16)
    outs[1][common : common + rows - common, :] = rest[:, :width].astype(jnp.bfloat16)
    outs[1][rows:, :] = rest[:, width:].astype(jnp.bfloat16)


def compact(pivots, pieces, weights, slot_count, row_count, part):
    _, rows, _ = pieces[0].shape
    width = pivots.shape[1]
    block_cols = (rows - part) * 2 // 3
    return pl.pallas_call(
        functools.partial(compact_kernel, weights, slot_count, row_count),
        out_shape=[
            jax.ShapeDtypeStruct((part + block_cols, width), jnp.bfloat16),
            jax.ShapeDtypeStruct((part + 2 * block_cols, width), jnp.bfloat16),
        ],
        in_specs=[pl.BlockSpec(memory_space=pltpu.VMEM)] * (1 + len(pieces)),
        out_specs=[pl.BlockSpec(memory_space=pltpu.VMEM)] * 2,
        compiler_params=pltpu.CompilerParams(vmem_limit_bytes=16 * MIB),
        cost_estimate=pl.CostEstimate(flops=MICRO, bytes_accessed=MIB, transcendentals=0),
        name="compact",
    )(pivots, *pieces)


def eliminate(block, columns, offset):
    vregs = LEAF // 8
    tiles = {g: [x[8 * v : 8 * v + 8] for v in range(vregs)] for g, x in block.items()}
    sublane = iota((8, LANES), 0)
    pivots = [jnp.zeros((8, LANES), jnp.float32) for _ in range(vregs)]
    for sub in range(0, LEAF, SUB):
        first = sub // 8
        diagonal = tiles[columns][first:]
        cols = [
            [
                jnp.broadcast_to(x[:, offset + sub + k : offset + sub + k + 1], (8, LANES))
                for x in diagonal
            ]
            for k in range(SUB)
        ]
        for j in range(SUB):
            jv, jr = j // 8, j % 8
            live = range(jv, len(diagonal))
            pivot = jnp.broadcast_to(cols[j][jv][jr : jr + 1, :], (8, LANES))
            inverse = 1.0 / pivot
            factor = {v: cols[j][v] * inverse for v in live}
            factor[jv] = jnp.where(sublane > jr, factor[jv], 0.0)
            pivots[first + jv] = jnp.where(sublane == jr, pivot, pivots[first + jv])
            for k in range(j + 1, SUB):
                entry = jnp.broadcast_to(cols[k][jv][jr : jr + 1, :], (8, LANES))
                for v in live:
                    cols[k][v] = cols[k][v] - factor[v] * entry
            for rows in tiles.values():
                entry = jnp.broadcast_to(rows[first + jv][jr : jr + 1, :], (8, LANES))
                for v in live:
                    rows[first + v] = rows[first + v] - factor[v] * entry
    scale = [lax.rsqrt(pivot) for pivot in pivots]
    return {
        g: jnp.concatenate([x * y for x, y in zip(rows, scale)], 0) for g, rows in tiles.items()
    }


def start_factor(matrix, work):
    width = matrix.shape[0]
    square = (width, width)
    work[:, :width] = 0.5 * (matrix + matrix.T)
    work[:, width:] = jnp.where(iota(square, 0) == iota(square, 1), 1.0, 0.0)


def lanes_of(g):
    return slice(g * LANES, (g + 1) * LANES)


def run_leaves(work, begin, end):
    width = work.shape[0]
    half = width // LANES
    block = None
    for start in range(begin, end, LEAF):
        following = start + LEAF
        rights = [half + g for g in range((following - 1) // LANES + 1)]
        groups = list(range(start // LANES, half)) + rights
        if block is None:
            block = {g: work[start:following, lanes_of(g)] for g in groups}
        upper = eliminate(block, start // LANES, start % LANES)
        for g in rights:
            work[start:following, lanes_of(g)] = upper[g]
        if following == width:
            break
        lefts = list(range(following // LANES, half))
        used = lefts + rights
        base = lefts[0] * LANES
        high, low = split(jnp.concatenate([upper[g] for g in used], 1))
        right = jnp.concatenate([high, high, low], 0)

        def product(first, last):
            a = high[:, first - base : last - base]
            b = low[:, first - base : last - base]
            return dot(jnp.concatenate([a, b, a], 0), right, 0, 0)

        stop = following + LEAF
        change = product(following, stop)
        block = {}
        for g in lefts + [half + g for g in range((stop - 1) // LANES + 1)]:
            block[g] = work[following:stop, lanes_of(g)]
            if g in used:
                block[g] = block[g] - change[:, lanes_of(used.index(g))]
        if following == end:
            for g, x in block.items():
                work[following:stop, lanes_of(g)] = x
        if stop < width:
            change = product(stop, width)
            for i, g in enumerate(used):
                work[stop:, lanes_of(g)] = work[stop:, lanes_of(g)] - change[:, lanes_of(i)]


def first_kernel(apart, part, *refs):
    count = len(apart)
    picked = refs[:count]
    work, rows_of, ints = refs[count:]
    me = lax.axis_index("cols")
    block_cols = picked[0].shape[0] - part
    for ref, bits in zip(picked, apart):
        at = pl.multiple_of((me ^ bits) * block_cols, block_cols)
        rows_of[pl.ds(pl.multiple_of((me ^ bits) * part, part), part), :] = ref[:part, :]
        ints[pl.ds(at, block_cols), :] = ref[part:, :].astype(jnp.float32)
    at_pivots = rows_of[...]
    start_factor(ints[...] - dot(at_pivots, at_pivots, 0, 0), work)
    run_leaves(work, 0, work.shape[0] // 2)


def first_half(picked, apart, part):
    count = len(apart)
    _, width = picked[0].shape
    return pl.pallas_call(
        functools.partial(first_kernel, apart, part),
        out_shape=jax.ShapeDtypeStruct((width, 2 * width), jnp.float32),
        in_specs=[pl.BlockSpec(memory_space=pltpu.VMEM)] * count,
        out_specs=pl.BlockSpec(memory_space=pltpu.VMEM),
        scratch_shapes=[
            pltpu.VMEM((count * part, width), jnp.bfloat16),
            pltpu.VMEM((width, width), jnp.float32),
        ],
        compiler_params=pltpu.CompilerParams(vmem_limit_bytes=16 * MIB),
        cost_estimate=pl.CostEstimate(flops=4 * MICRO, bytes_accessed=MIB, transcendentals=0),
        name="first_half",
    )(*picked)


def second_kernel(before_ref, work):
    work[...] = before_ref[...]
    run_leaves(work, work.shape[0] // 2, work.shape[0])


def second_half(work):
    return pl.pallas_call(
        second_kernel,
        out_shape=jax.ShapeDtypeStruct(work.shape, work.dtype),
        in_specs=[pl.BlockSpec(memory_space=pltpu.VMEM)],
        out_specs=pl.BlockSpec(memory_space=pltpu.VMEM),
        compiler_params=pltpu.CompilerParams(vmem_limit_bytes=16 * MIB),
        cost_estimate=pl.CostEstimate(flops=4 * MICRO, bytes_accessed=MIB, transcendentals=0),
        name="second_half",
    )(work)


def third_kernel(apart, part, *refs):
    count = len(apart)
    work0, picked0, picked1 = refs[0], refs[1 : 1 + count], refs[1 + count : 1 + 2 * count]
    work1, rows_of, ahead_ref, ints0, ints1 = refs[1 + 2 * count :]
    me = lax.axis_index("cols")
    width = work0.shape[0]
    block_cols = picked0[0].shape[0] - part
    for i, bits in enumerate(apart):
        at = pl.ds(pl.multiple_of((me ^ bits) * part, part), part)
        rows_of[at, :width] = picked0[i][:part, :]
        rows_of[at, width:] = picked1[i][:part, :]
        at = pl.ds(pl.multiple_of((me ^ bits) * block_cols, block_cols), block_cols)
        ints0[at, :] = picked1[i][part : part + block_cols, :].astype(jnp.float32)
        ints1[at, :] = picked1[i][part + block_cols :, :].astype(jnp.float32)
    gram = dot(rows_of[...], rows_of[:, width:], 0, 0)
    ahead = product_wide(work0[:, width:], ints0[...] - gram[:width]).astype(jnp.bfloat16)
    ahead_ref[...] = ahead
    start_factor(ints1[...] - gram[width:] - dot(ahead, ahead, 0, 0), work1)
    run_leaves(work1, 0, width // 2)


def third_half(work0, picked0, picked1, apart, part):
    count = len(apart)
    width = work0.shape[0]
    return pl.pallas_call(
        functools.partial(third_kernel, apart, part),
        out_shape=[
            jax.ShapeDtypeStruct(work0.shape, jnp.float32),
            jax.ShapeDtypeStruct((count * part, 2 * width), jnp.bfloat16),
            jax.ShapeDtypeStruct((width, width), jnp.bfloat16),
        ],
        in_specs=[pl.BlockSpec(memory_space=pltpu.VMEM)] * (1 + 2 * count),
        out_specs=[pl.BlockSpec(memory_space=pltpu.VMEM)] * 3,
        scratch_shapes=[pltpu.VMEM((width, width), jnp.float32)] * 2,
        compiler_params=pltpu.CompilerParams(vmem_limit_bytes=16 * MIB),
        cost_estimate=pl.CostEstimate(flops=5 * MICRO, bytes_accessed=MIB, transcendentals=0),
        name="third_half",
    )(work0, *picked0, *picked1)


def fourth_kernel(block_cols, work0, before_ref, rows_of, ahead, left, work1):
    width = work0.shape[0]
    both = 2 * width
    work1[...] = before_ref[...]
    run_leaves(work1, width // 2, width)
    me = lax.axis_index("cols")
    mine = pl.ds(pl.multiple_of(me * block_cols, block_cols), block_cols)
    inverse0 = work0[mine, width:]
    inverse1 = work1[mine, width:]
    through = product_wide(product_narrow(inverse1, ahead[...], 1), work0[:, width:])
    small = jnp.concatenate(
        [
            jnp.concatenate([inverse0, jnp.zeros_like(inverse0)], 1),
            jnp.concatenate([-through, inverse1], 1),
        ],
        0,
    )
    left[:, :both] = jnp.concatenate(split(small), 0)
    left[:, both:] = jnp.concatenate(split(-product_narrow(small, rows_of[...], 1)), 0)


def fourth_half(work0, work1, rows_of, ahead, block_cols):
    width = work0.shape[0]
    return pl.pallas_call(
        functools.partial(fourth_kernel, block_cols),
        out_shape=jax.ShapeDtypeStruct(
            (4 * block_cols, 2 * width + rows_of.shape[0]), jnp.bfloat16
        ),
        in_specs=[pl.BlockSpec(memory_space=pltpu.VMEM)] * 4,
        out_specs=pl.BlockSpec(memory_space=pltpu.VMEM),
        scratch_shapes=[pltpu.VMEM(work0.shape, jnp.float32)],
        compiler_params=pltpu.CompilerParams(vmem_limit_bytes=16 * MIB),
        cost_estimate=pl.CostEstimate(flops=5 * MICRO, bytes_accessed=MIB, transcendentals=0),
        name="fourth_half",
    )(work0, work1, rows_of, ahead)


def finish_kernel(apart, *refs):
    count = len(apart)
    left, vectors_ref = refs[0], refs[1]
    blocks = refs[2 : 2 + 2 * count]
    out_ref, right, result, sems, out_sems = refs[2 + 2 * count :]
    me = lax.axis_index("cols")
    pairs = vectors_ref.shape[1]
    block_cols = blocks[0].shape[0]
    both = right.shape[0]
    copies = []
    for n in range(pairs // CHUNK):
        for i, ref in enumerate(blocks):
            place = i // count * (both // 2) + (me ^ apart[i % count]) * block_cols
            rows = pl.ds(pl.multiple_of(place, block_cols), block_cols)
            at = pl.ds(n * CHUNK, CHUNK)
            copies.append(
                pltpu.make_async_copy(ref.at[:, at], right.at[rows, at], sems.at[n, i])
            )
            copies[-1].start()
    outs = []
    for n in range(pairs // CHUNK):
        at = pl.ds(n * CHUNK, CHUNK)
        for copy in copies[n * len(blocks) : (n + 1) * len(blocks)]:
            copy.wait()
        halves = dot(left[:, both:], vectors_ref[:, at]) + dot(left[:, :both], right[:, at])
        value = halves[: 2 * block_cols] + halves[2 * block_cols :]
        result[0, :, at] = value[:block_cols]
        result[1, :, at] = value[block_cols:]
        outs.append(
            pltpu.make_async_copy(result.at[:, :, at], out_ref.at[:, :, at], out_sems.at[n])
        )
        outs[-1].start()
    for copy in outs:
        copy.wait()


def finish(left, vectors, blocks, apart):
    block_cols, pairs = blocks[0].shape
    both = left.shape[1] - vectors.shape[0]
    return pl.pallas_call(
        functools.partial(finish_kernel, apart),
        out_shape=jax.ShapeDtypeStruct((2, block_cols, pairs), jnp.float32),
        in_specs=[pl.BlockSpec(memory_space=pltpu.VMEM)] * 2
        + [pl.BlockSpec(memory_space=pl.ANY)] * len(blocks),
        out_specs=pl.BlockSpec(memory_space=pl.ANY),
        scratch_shapes=[
            pltpu.VMEM((both, pairs), jnp.bfloat16),
            pltpu.VMEM((2, block_cols, pairs), jnp.float32),
            pltpu.SemaphoreType.DMA((pairs // CHUNK, len(blocks))),
            pltpu.SemaphoreType.DMA((pairs // CHUNK,)),
        ],
        compiler_params=pltpu.CompilerParams(vmem_limit_bytes=24 * MIB),
        cost_estimate=pl.CostEstimate(
            flops=6 * MICRO, bytes_accessed=16 * MIB, transcendentals=0
        ),
        name="finish",
    )(left, vectors, *blocks)


def per_device(vectors, integrals, pivots):
    prior, row_count = vectors.shape
    _, width = pivots.shape
    owners, col_count = lax.axis_size("rows"), lax.axis_size("cols")
    block_cols = integrals.shape[1]
    slot_count = 2 * width // owners
    part = prior // col_count

    def swap(x, axis, mask):
        size = lax.axis_size(axis)
        return lax.ppermute(x, axis, [(i, i ^ mask) for i in range(size)])

    def near(pieces):
        return [swap(piece, "cols", near_mask) for piece in pieces]

    far_mask, near_mask = masks_of(col_count)
    apart = [0, far_mask, near_mask, far_mask ^ near_mask]

    found, ints = select(pivots, vectors, integrals, slot_count, part)
    masks = masks_of(owners)
    held = found[None]
    depth, weights = 1, []
    for mask in masks[:-3]:
        held = jnp.concatenate([held, swap(held, "rows", mask)], 0)
        weights.append((mask, depth))
        depth = 2 * depth
    weights += [(mask, depth << i) for i, mask in enumerate(masks[-3:])]
    passed = swap(held, "rows", masks[-3])
    pieces = [held, passed]
    for mask in (masks[-2], masks[-1], masks[-2] ^ masks[-1]):
        pieces.append(swap(held, "rows", mask))
        pieces.append(swap(passed, "rows", mask))
    own0, own1 = compact(pivots, pieces, weights, slot_count, row_count, part)

    far0 = swap(ints[0], "cols", far_mask)
    other0 = swap(own0, "cols", far_mask)
    other1 = swap(own1, "cols", far_mask)
    pair1 = [own1, other1]
    picked0 = [own0, other0] + near([own0]) + near([other0])
    picked0, last = lax.optimization_barrier((picked0, ints[1]))
    far1 = swap(last, "cols", far_mask)
    work0 = first_half(picked0, apart, part)
    work0, pair1, ints0 = lax.optimization_barrier((work0, pair1, [ints[0], far0]))
    picked1 = pair1 + near(pair1)
    blocks = ints0 + near(ints0)
    work0 = second_half(work0)
    work1, rows_of, ahead = third_half(work0, picked0, picked1, apart, part)
    work1, ints1 = lax.optimization_barrier((work1, [last, far1]))
    blocks += ints1 + near(ints1)
    left = fourth_half(work0, work1, rows_of, ahead, block_cols)
    return finish(left, vectors, blocks, apart)


def solution(mesh):
    placed = (P(None, "rows"), P(None, "cols", "rows"), P())

    return jax.shard_map(
        per_device, mesh=mesh, in_specs=placed, out_specs=P(None, "cols", "rows"), check_vma=False
    )
```

```python
import functools

import jax
import jax.numpy as jnp
from jax import lax
from jax.experimental import pallas as pl
from jax.experimental.pallas import tpu as pltpu
from jax.sharding import PartitionSpec as P

LANES = 128
LEAF = 32
SUB = 16
CHUNK = 1024
SELECT = 512
MICRO = 1 << 29
MIB = 1 << 20
ALMOST_ALL = 52 * MIB


def masks_of(size):
    return [1 << bit for bit in reversed(range(size.bit_length() - 1))]


def dot(left, right, left_dim=1, right_dim=0):
    return lax.dot_general(
        left, right, (((left_dim,), (right_dim,)), ((), ())), preferred_element_type=jnp.float32
    )


def split(x):
    high = x.astype(jnp.bfloat16)
    return high, (x - high.astype(jnp.float32)).astype(jnp.bfloat16)


def product_narrow(left, right, right_dim=0):
    rows = left.shape[0]
    both = dot(jnp.concatenate(split(left), 0), right, 1, right_dim)
    return both[:rows] + both[rows:]


def product_wide(left, right):
    left_high, left_low = split(left)
    right_high, right_low = split(right)
    return dot(
        jnp.concatenate([left_high, left_low, left_high], 1),
        jnp.concatenate([right_high, right_high, right_low], 0),
    )


def iota(shape, dim):
    return lax.broadcasted_iota(jnp.int32, shape, dim)


def as_column(row):
    size = row.shape[1]
    square = (size, size)
    return jnp.sum(
        jnp.where(iota(square, 0) == iota(square, 1), jnp.broadcast_to(row, square), 0.0),
        axis=1,
        keepdims=True,
    )


def pack(x):
    half = x.shape[0] // 2
    return jnp.concatenate([x[:half], x[half:]], 1)


def select_kernel(slot_count, pivots_ref, vectors_ref, integrals_ref, *refs):
    panels, block_cols, _ = integrals_ref.shape
    found_ref, out_refs = refs[0], refs[1 : 1 + panels]
    vec, ints, local_pivots, sems = refs[1 + panels :]
    part, row_count = vec.shape
    width = pivots_ref.shape[1]
    listed = pltpu.make_async_copy(pivots_ref, local_pivots, sems.at[sems.shape[0] - 1])
    listed.start()
    lanes = panels * slot_count
    first = pl.multiple_of(lax.axis_index("cols") * part, part)
    step = min(SELECT, row_count)
    count = row_count // step
    copies = []
    for n in range(count):
        at = pl.ds(n * step, step)
        copies.append(
            pltpu.make_async_copy(
                vectors_ref.at[pl.ds(first, part), at], vec.at[:, at], sems.at[n]
            )
        )
    whole = pltpu.make_async_copy(integrals_ref, ints, sems.at[count])
    for copy in copies[:1] + [whole] + copies[1:]:
        copy.start()
    listed.wait()
    start = (lax.axis_index("rows") * row_count).astype(jnp.float32)
    square = (width, width)
    target = jnp.zeros((1, lanes), jnp.float32)
    for panel in range(panels):
        local = local_pivots[panel : panel + 1, :].astype(jnp.float32) - start
        mine = ((local >= 0.0) & (local < row_count)).astype(jnp.float32)
        earlier = iota(square, 1) < iota(square, 0)
        rank = jnp.sum(
            jnp.where(earlier, jnp.broadcast_to(mine, square), 0.0), axis=1, keepdims=True
        )
        held = as_column(jnp.where(mine > 0.0, local + 1.0, 0.0))
        slot = iota((width, lanes), 1).astype(jnp.float32) - panel * slot_count
        target = target + jnp.sum(jnp.where(rank == slot, held, 0.0), axis=0, keepdims=True)
    target = target.astype(jnp.int32) - 1
    whole.wait()
    outs = [
        pltpu.make_async_copy(ints.at[panel], out_refs[panel], sems.at[count + 1 + panel])
        for panel in range(panels)
    ]
    for copy in outs:
        copy.start()
    found = jnp.zeros((part + panels * block_cols, lanes), jnp.float32)
    for n, copy in enumerate(copies):
        copy.wait()
        at = slice(n * step, (n + 1) * step)
        pick = jnp.where(iota((step, lanes), 0) + n * step == target, 1.0, 0.0).astype(jnp.bfloat16)
        left = jnp.concatenate([vec[:, at]] + [ints[panel, :, at] for panel in range(panels)], 0)
        found = found + dot(left, pick)
    common = part + block_cols
    found_ref[:common, :] = found[:common].astype(jnp.bfloat16)
    found_ref[common:, :] = pack(found[common:, slot_count:]).astype(jnp.bfloat16)
    for copy in outs:
        copy.wait()


def select(pivots, vectors, integrals, slot_count, part):
    panels, block_cols, row_count = integrals.shape
    rows = part + block_cols + block_cols // 2
    outs = [jax.ShapeDtypeStruct((rows, panels * slot_count), jnp.bfloat16)]
    outs += [jax.ShapeDtypeStruct((block_cols, row_count), jnp.bfloat16)] * panels
    results = pl.pallas_call(
        functools.partial(select_kernel, slot_count),
        out_shape=outs,
        in_specs=[pl.BlockSpec(memory_space=pl.ANY)] * 3,
        out_specs=[pl.BlockSpec(memory_space=pltpu.VMEM)]
        + [pl.BlockSpec(memory_space=pltpu.HBM)] * panels,
        scratch_shapes=[
            pltpu.VMEM((part, row_count), jnp.bfloat16),
            pltpu.VMEM(integrals.shape, jnp.bfloat16),
            pltpu.VMEM(pivots.shape, jnp.int32),
            pltpu.SemaphoreType.DMA((row_count // min(SELECT, row_count) + 2 + panels,)),
        ],
        compiler_params=pltpu.CompilerParams(vmem_limit_bytes=ALMOST_ALL),
        cost_estimate=pl.CostEstimate(flops=MICRO * 2, bytes_accessed=3 * MIB, transcendentals=0),
        name="select",
    )(pivots, vectors, integrals)
    return results[0], results[1:]


def compact_kernel(weights, slot_count, row_count, pivots_ref, *refs):
    pieces, outs = refs[:-2], refs[-2:]
    panels, width = pivots_ref.shape
    depth, rows, lanes = pieces[0].shape
    common = outs[0].shape[0]
    shift = row_count.bit_length() - 1
    me = lax.axis_index("rows")
    square = (width, width)
    places = []
    for panel in range(panels):
        owner = lax.shift_right_logical(
            pivots_ref[panel : panel + 1, :], jnp.full((1, width), shift, jnp.int32)
        )
        floats = owner.astype(jnp.float32)
        same = jnp.broadcast_to(floats, square) == as_column(floats)
        earlier = iota(square, 0) < iota(square, 1)
        rank = jnp.sum(
            jnp.where(same & earlier, 1.0, 0.0), axis=0, keepdims=True
        ).astype(jnp.int32)
        apart = owner ^ me
        block = jnp.zeros_like(owner)
        for mask, weight in weights:
            block = block + jnp.where((apart & mask) != 0, weight, 0)
        places.append(block * lanes + rank)
    both = jnp.concatenate([places[0], places[1] + slot_count], 1)
    halves = jnp.concatenate([places[1], places[1] + slot_count], 1)
    main = jnp.zeros((common, 2 * width), jnp.float32)
    rest = jnp.zeros((rows - common, 2 * width), jnp.float32)
    for i in range(len(pieces) * depth):
        lane = iota((lanes, 2 * width), 0) + i * lanes
        x = pieces[i // depth][i % depth]
        main = main + dot(x[:common], jnp.where(lane == both, 1.0, 0.0).astype(jnp.bfloat16))
        rest = rest + dot(x[common:], jnp.where(lane == halves, 1.0, 0.0).astype(jnp.bfloat16))
    outs[0][...] = main[:, :width].astype(jnp.bfloat16)
    outs[1][:common, :] = main[:, width:].astype(jnp.bfloat16)
    outs[1][common : common + rows - common, :] = rest[:, :width].astype(jnp.bfloat16)
    outs[1][rows:, :] = rest[:, width:].astype(jnp.bfloat16)


def compact(pivots, pieces, weights, slot_count, row_count, part):
    _, rows, _ = pieces[0].shape
    width = pivots.shape[1]
    block_cols = (rows - part) * 2 // 3
    return pl.pallas_call(
        functools.partial(compact_kernel, weights, slot_count, row_count),
        out_shape=[
            jax.ShapeDtypeStruct((part + block_cols, width), jnp.bfloat16),
            jax.ShapeDtypeStruct((part + 2 * block_cols, width), jnp.bfloat16),
        ],
        in_specs=[pl.BlockSpec(memory_space=pltpu.VMEM)] * (1 + len(pieces)),
        out_specs=[pl.BlockSpec(memory_space=pltpu.VMEM)] * 2,
        compiler_params=pltpu.CompilerParams(vmem_limit_bytes=16 * MIB),
        cost_estimate=pl.CostEstimate(flops=MICRO, bytes_accessed=MIB, transcendentals=0),
        name="compact",
    )(pivots, *pieces)


def eliminate(block, columns, offset):
    vregs = LEAF // 8
    tiles = {g: [x[8 * v : 8 * v + 8] for v in range(vregs)] for g, x in block.items()}
    sublane = iota((8, LANES), 0)
    pivots = [jnp.zeros((8, LANES), jnp.float32) for _ in range(vregs)]
    for sub in range(0, LEAF, SUB):
        first = sub // 8
        diagonal = tiles[columns][first:]
        cols = [
            [
                jnp.broadcast_to(x[:, offset + sub + k : offset + sub + k + 1], (8, LANES))
                for x in diagonal
            ]
            for k in range(SUB)
        ]
        for j in range(SUB):
            jv, jr = j // 8, j % 8
            live = range(jv, len(diagonal))
            pivot = jnp.broadcast_to(cols[j][jv][jr : jr + 1, :], (8, LANES))
            inverse = 1.0 / pivot
            factor = {v: cols[j][v] * inverse for v in live}
            factor[jv] = jnp.where(sublane > jr, factor[jv], 0.0)
            pivots[first + jv] = jnp.where(sublane == jr, pivot, pivots[first + jv])
            for k in range(j + 1, SUB):
                entry = jnp.broadcast_to(cols[k][jv][jr : jr + 1, :], (8, LANES))
                for v in live:
                    cols[k][v] = cols[k][v] - factor[v] * entry
            for rows in tiles.values():
                entry = jnp.broadcast_to(rows[first + jv][jr : jr + 1, :], (8, LANES))
                for v in live:
                    rows[first + v] = rows[first + v] - factor[v] * entry
    scale = [lax.rsqrt(pivot) for pivot in pivots]
    return {
        g: jnp.concatenate([x * y for x, y in zip(rows, scale)], 0) for g, rows in tiles.items()
    }


def start_factor(matrix, work):
    width = matrix.shape[0]
    square = (width, width)
    work[:, :width] = 0.5 * (matrix + matrix.T)
    work[:, width:] = jnp.where(iota(square, 0) == iota(square, 1), 1.0, 0.0)


def lanes_of(g):
    return slice(g * LANES, (g + 1) * LANES)


def run_leaves(work, begin, end):
    width = work.shape[0]
    half = width // LANES
    block = None
    for start in range(begin, end, LEAF):
        following = start + LEAF
        rights = [half + g for g in range((following - 1) // LANES + 1)]
        groups = list(range(start // LANES, half)) + rights
        if block is None:
            block = {g: work[start:following, lanes_of(g)] for g in groups}
        upper = eliminate(block, start // LANES, start % LANES)
        for g in rights:
            work[start:following, lanes_of(g)] = upper[g]
        if following == width:
            break
        lefts = list(range(following // LANES, half))
        used = lefts + rights
        base = lefts[0] * LANES
        high, low = split(jnp.concatenate([upper[g] for g in used], 1))
        right = jnp.concatenate([high, high, low], 0)

        def product(first, last):
            a = high[:, first - base : last - base]
            b = low[:, first - base : last - base]
            return dot(jnp.concatenate([a, b, a], 0), right, 0, 0)

        stop = following + LEAF
        change = product(following, stop)
        block = {}
        for g in lefts + [half + g for g in range((stop - 1) // LANES + 1)]:
            block[g] = work[following:stop, lanes_of(g)]
            if g in used:
                block[g] = block[g] - change[:, lanes_of(used.index(g))]
        if following == end:
            for g, x in block.items():
                work[following:stop, lanes_of(g)] = x
        if stop < width:
            change = product(stop, width)
            for i, g in enumerate(used):
                work[stop:, lanes_of(g)] = work[stop:, lanes_of(g)] - change[:, lanes_of(i)]


def first_kernel(apart, part, *refs):
    count = len(apart)
    picked = refs[:count]
    work, rows_of, ints = refs[count:]
    me = lax.axis_index("cols")
    block_cols = picked[0].shape[0] - part
    for ref, bits in zip(picked, apart):
        at = pl.multiple_of((me ^ bits) * block_cols, block_cols)
        rows_of[pl.ds(pl.multiple_of((me ^ bits) * part, part), part), :] = ref[:part, :]
        ints[pl.ds(at, block_cols), :] = ref[part:, :].astype(jnp.float32)
    at_pivots = rows_of[...]
    start_factor(ints[...] - dot(at_pivots, at_pivots, 0, 0), work)
    run_leaves(work, 0, work.shape[0] // 2)


def first_half(picked, apart, part):
    count = len(apart)
    _, width = picked[0].shape
    return pl.pallas_call(
        functools.partial(first_kernel, apart, part),
        out_shape=jax.ShapeDtypeStruct((width, 2 * width), jnp.float32),
        in_specs=[pl.BlockSpec(memory_space=pltpu.VMEM)] * count,
        out_specs=pl.BlockSpec(memory_space=pltpu.VMEM),
        scratch_shapes=[
            pltpu.VMEM((count * part, width), jnp.bfloat16),
            pltpu.VMEM((width, width), jnp.float32),
        ],
        compiler_params=pltpu.CompilerParams(vmem_limit_bytes=16 * MIB),
        cost_estimate=pl.CostEstimate(flops=4 * MICRO, bytes_accessed=MIB, transcendentals=0),
        name="first_half",
    )(*picked)


def second_kernel(before_ref, work):
    work[...] = before_ref[...]
    run_leaves(work, work.shape[0] // 2, work.shape[0])


def second_half(work):
    return pl.pallas_call(
        second_kernel,
        out_shape=jax.ShapeDtypeStruct(work.shape, work.dtype),
        in_specs=[pl.BlockSpec(memory_space=pltpu.VMEM)],
        out_specs=pl.BlockSpec(memory_space=pltpu.VMEM),
        compiler_params=pltpu.CompilerParams(vmem_limit_bytes=16 * MIB),
        cost_estimate=pl.CostEstimate(flops=4 * MICRO, bytes_accessed=MIB, transcendentals=0),
        name="second_half",
    )(work)


def third_kernel(apart, part, *refs):
    count = len(apart)
    work0, picked0, picked1 = refs[0], refs[1 : 1 + count], refs[1 + count : 1 + 2 * count]
    work1, rows_of, ahead_ref, ints0, ints1 = refs[1 + 2 * count :]
    me = lax.axis_index("cols")
    width = work0.shape[0]
    block_cols = picked0[0].shape[0] - part
    for i, bits in enumerate(apart):
        at = pl.ds(pl.multiple_of((me ^ bits) * part, part), part)
        rows_of[at, :width] = picked0[i][:part, :]
        rows_of[at, width:] = picked1[i][:part, :]
        at = pl.ds(pl.multiple_of((me ^ bits) * block_cols, block_cols), block_cols)
        ints0[at, :] = picked1[i][part : part + block_cols, :].astype(jnp.float32)
        ints1[at, :] = picked1[i][part + block_cols :, :].astype(jnp.float32)
    gram = dot(rows_of[...], rows_of[:, width:], 0, 0)
    ahead = product_wide(work0[:, width:], ints0[...] - gram[:width]).astype(jnp.bfloat16)
    ahead_ref[...] = ahead
    start_factor(ints1[...] - gram[width:] - dot(ahead, ahead, 0, 0), work1)
    run_leaves(work1, 0, width // 2)


def third_half(work0, picked0, picked1, apart, part):
    count = len(apart)
    width = work0.shape[0]
    return pl.pallas_call(
        functools.partial(third_kernel, apart, part),
        out_shape=[
            jax.ShapeDtypeStruct(work0.shape, jnp.float32),
            jax.ShapeDtypeStruct((count * part, 2 * width), jnp.bfloat16),
            jax.ShapeDtypeStruct((width, width), jnp.bfloat16),
        ],
        in_specs=[pl.BlockSpec(memory_space=pltpu.VMEM)] * (1 + 2 * count),
        out_specs=[pl.BlockSpec(memory_space=pltpu.VMEM)] * 3,
        scratch_shapes=[pltpu.VMEM((width, width), jnp.float32)] * 2,
        compiler_params=pltpu.CompilerParams(vmem_limit_bytes=16 * MIB),
        cost_estimate=pl.CostEstimate(flops=5 * MICRO, bytes_accessed=MIB, transcendentals=0),
        name="third_half",
    )(work0, *picked0, *picked1)


def fourth_kernel(block_cols, work0, before_ref, rows_of, ahead, left, work1):
    width = work0.shape[0]
    both = 2 * width
    work1[...] = before_ref[...]
    run_leaves(work1, width // 2, width)
    me = lax.axis_index("cols")
    mine = pl.ds(pl.multiple_of(me * block_cols, block_cols), block_cols)
    inverse0 = work0[mine, width:]
    inverse1 = work1[mine, width:]
    through = product_wide(product_narrow(inverse1, ahead[...], 1), work0[:, width:])
    small = jnp.concatenate(
        [
            jnp.concatenate([inverse0, jnp.zeros_like(inverse0)], 1),
            jnp.concatenate([-through, inverse1], 1),
        ],
        0,
    )
    left[:, :both] = jnp.concatenate(split(small), 0)
    left[:, both:] = jnp.concatenate(split(-product_narrow(small, rows_of[...], 1)), 0)


def fourth_half(work0, work1, rows_of, ahead, block_cols):
    width = work0.shape[0]
    return pl.pallas_call(
        functools.partial(fourth_kernel, block_cols),
        out_shape=jax.ShapeDtypeStruct(
            (4 * block_cols, 2 * width + rows_of.shape[0]), jnp.bfloat16
        ),
        in_specs=[pl.BlockSpec(memory_space=pltpu.VMEM)] * 4,
        out_specs=pl.BlockSpec(memory_space=pltpu.VMEM),
        scratch_shapes=[pltpu.VMEM(work0.shape, jnp.float32)],
        compiler_params=pltpu.CompilerParams(vmem_limit_bytes=16 * MIB),
        cost_estimate=pl.CostEstimate(flops=5 * MICRO, bytes_accessed=MIB, transcendentals=0),
        name="fourth_half",
    )(work0, work1, rows_of, ahead)


def finish_kernel(apart, *refs):
    count = len(apart)
    left, vectors_ref = refs[0], refs[1]
    blocks = refs[2 : 2 + 2 * count]
    out_ref, right, result, out_sems = refs[2 + 2 * count :]
    me = lax.axis_index("cols")
    pairs = vectors_ref.shape[1]
    block_cols = blocks[0].shape[0]
    both = right.shape[0]
    outs = []
    for n in range(pairs // CHUNK):
        at = slice(n * CHUNK, (n + 1) * CHUNK)
        for i, ref in enumerate(blocks):
            place = i // count * (both // 2) + (me ^ apart[i % count]) * block_cols
            right[pl.ds(pl.multiple_of(place, block_cols), block_cols), :] = ref[:, at]
        halves = dot(left[:, both:], vectors_ref[:, at]) + dot(left[:, :both], right[...])
        value = halves[: 2 * block_cols] + halves[2 * block_cols :]
        result[0, :, at] = value[:block_cols]
        result[1, :, at] = value[block_cols:]
        outs.append(
            pltpu.make_async_copy(result.at[:, :, at], out_ref.at[:, :, at], out_sems.at[n])
        )
        outs[-1].start()
    for copy in outs:
        copy.wait()


def finish(left, vectors, blocks, apart):
    block_cols, pairs = blocks[0].shape
    both = left.shape[1] - vectors.shape[0]
    return pl.pallas_call(
        functools.partial(finish_kernel, apart),
        out_shape=jax.ShapeDtypeStruct((2, block_cols, pairs), jnp.float32),
        in_specs=[pl.BlockSpec(memory_space=pltpu.VMEM)] * (2 + len(blocks)),
        out_specs=pl.BlockSpec(memory_space=pl.ANY),
        scratch_shapes=[
            pltpu.VMEM((both, CHUNK), jnp.bfloat16),
            pltpu.VMEM((2, block_cols, pairs), jnp.float32),
            pltpu.SemaphoreType.DMA((pairs // CHUNK,)),
        ],
        compiler_params=pltpu.CompilerParams(vmem_limit_bytes=24 * MIB),
        cost_estimate=pl.CostEstimate(
            flops=6 * MICRO, bytes_accessed=16 * MIB, transcendentals=0
        ),
        name="finish",
    )(left, vectors, *blocks)


def per_device(vectors, integrals, pivots):
    prior, row_count = vectors.shape
    _, width = pivots.shape
    owners, col_count = lax.axis_size("rows"), lax.axis_size("cols")
    block_cols = integrals.shape[1]
    slot_count = 2 * width // owners
    part = prior // col_count

    def swap(x, axis, mask):
        size = lax.axis_size(axis)
        return lax.ppermute(x, axis, [(i, i ^ mask) for i in range(size)])

    def near(pieces):
        return [swap(piece, "cols", near_mask) for piece in pieces]

    far_mask, near_mask = masks_of(col_count)
    apart = [0, far_mask, near_mask, far_mask ^ near_mask]

    found, ints = select(pivots, vectors, integrals, slot_count, part)
    masks = masks_of(owners)
    held = found[None]
    depth, weights = 1, []
    for mask in masks[:-3]:
        held = jnp.concatenate([held, swap(held, "rows", mask)], 0)
        weights.append((mask, depth))
        depth = 2 * depth
    weights += [(mask, depth << i) for i, mask in enumerate(masks[-3:])]
    passed = swap(held, "rows", masks[-3])
    pieces = [held, passed]
    for mask in (masks[-2], masks[-1], masks[-2] ^ masks[-1]):
        pieces.append(swap(held, "rows", mask))
        pieces.append(swap(passed, "rows", mask))
    own0, own1 = compact(pivots, pieces, weights, slot_count, row_count, part)

    far0 = swap(ints[0], "cols", far_mask)
    other0 = swap(own0, "cols", far_mask)
    other1 = swap(own1, "cols", far_mask)
    picked0 = [own0, other0] + near([own0]) + near([other0])
    beside1 = near([own1])
    beside = near(ints)
    picked0, last = lax.optimization_barrier((picked0, ints[1]))
    far1 = swap(last, "cols", far_mask)
    work0 = first_half(picked0, apart, part)
    work0, other1, far0 = lax.optimization_barrier((work0, other1, far0))
    picked1 = [own1, other1] + beside1 + near([other1])
    blocks = [ints[0], far0, beside[0]] + near([far0])
    work0 = second_half(work0)
    work1, rows_of, ahead = third_half(work0, picked0, picked1, apart, part)
    work1, far1 = lax.optimization_barrier((work1, far1))
    blocks += [last, far1, beside[1]] + near([far1])
    left = fourth_half(work0, work1, rows_of, ahead, block_cols)
    return finish(left, vectors, blocks, apart)


def solution(mesh):
    placed = (P(None, "rows"), P(None, "cols", "rows"), P())

    return jax.shard_map(
        per_device, mesh=mesh, in_specs=placed, out_specs=P(None, "cols", "rows"), check_vma=False
    )
```

```python
import functools

import jax
import jax.numpy as jnp
from jax import lax
from jax.experimental import pallas as pl
from jax.experimental.pallas import tpu as pltpu
from jax.sharding import PartitionSpec as P

LANES = 128
LEAF = 32
SUB = 16
CHUNK = 512
SELECT = 512
MICRO = 1 << 29
MIB = 1 << 20
ALMOST_ALL = 52 * MIB


def masks_of(size):
    return [1 << bit for bit in reversed(range(size.bit_length() - 1))]


def dot(left, right, left_dim=1, right_dim=0):
    return lax.dot_general(
        left, right, (((left_dim,), (right_dim,)), ((), ())), preferred_element_type=jnp.float32
    )


def split(x):
    high = x.astype(jnp.bfloat16)
    return high, (x - high.astype(jnp.float32)).astype(jnp.bfloat16)


def product_narrow(left, right, right_dim=0):
    rows = left.shape[0]
    both = dot(jnp.concatenate(split(left), 0), right, 1, right_dim)
    return both[:rows] + both[rows:]


def product_wide(left, right):
    left_high, left_low = split(left)
    right_high, right_low = split(right)
    return dot(
        jnp.concatenate([left_high, left_low, left_high], 1),
        jnp.concatenate([right_high, right_high, right_low], 0),
    )


def iota(shape, dim):
    return lax.broadcasted_iota(jnp.int32, shape, dim)


def as_column(row):
    size = row.shape[1]
    square = (size, size)
    return jnp.sum(
        jnp.where(iota(square, 0) == iota(square, 1), jnp.broadcast_to(row, square), 0.0),
        axis=1,
        keepdims=True,
    )


def pack(x):
    half = x.shape[0] // 2
    return jnp.concatenate([x[:half], x[half:]], 1)


def select_kernel(slot_count, pivots_ref, vectors_ref, integrals_ref, *refs):
    panels, block_cols, _ = integrals_ref.shape
    found_ref, out_refs = refs[0], refs[1 : 1 + panels]
    vec, ints, local_pivots, sems = refs[1 + panels :]
    part, row_count = vec.shape
    width = pivots_ref.shape[1]
    listed = pltpu.make_async_copy(pivots_ref, local_pivots, sems.at[sems.shape[0] - 1])
    listed.start()
    lanes = panels * slot_count
    first = pl.multiple_of(lax.axis_index("cols") * part, part)
    step = min(SELECT, row_count)
    count = row_count // step
    copies = []
    for n in range(count):
        at = pl.ds(n * step, step)
        copies.append(
            pltpu.make_async_copy(
                vectors_ref.at[pl.ds(first, part), at], vec.at[:, at], sems.at[n]
            )
        )
    whole = pltpu.make_async_copy(integrals_ref, ints, sems.at[count])
    for copy in copies[:1] + [whole] + copies[1:]:
        copy.start()
    listed.wait()
    start = (lax.axis_index("rows") * row_count).astype(jnp.float32)
    square = (width, width)
    target = jnp.zeros((1, lanes), jnp.float32)
    for panel in range(panels):
        local = local_pivots[panel : panel + 1, :].astype(jnp.float32) - start
        mine = ((local >= 0.0) & (local < row_count)).astype(jnp.float32)
        earlier = iota(square, 1) < iota(square, 0)
        rank = jnp.sum(
            jnp.where(earlier, jnp.broadcast_to(mine, square), 0.0), axis=1, keepdims=True
        )
        held = as_column(jnp.where(mine > 0.0, local + 1.0, 0.0))
        slot = iota((width, lanes), 1).astype(jnp.float32) - panel * slot_count
        target = target + jnp.sum(jnp.where(rank == slot, held, 0.0), axis=0, keepdims=True)
    target = target.astype(jnp.int32) - 1
    whole.wait()
    outs = [
        pltpu.make_async_copy(ints.at[panel], out_refs[panel], sems.at[count + 1 + panel])
        for panel in range(panels)
    ]
    for copy in outs:
        copy.start()
    found = jnp.zeros((part + panels * block_cols, lanes), jnp.float32)
    for n, copy in enumerate(copies):
        copy.wait()
        at = slice(n * step, (n + 1) * step)
        pick = jnp.where(iota((step, lanes), 0) + n * step == target, 1.0, 0.0).astype(jnp.bfloat16)
        left = jnp.concatenate([vec[:, at]] + [ints[panel, :, at] for panel in range(panels)], 0)
        found = found + dot(left, pick)
    common = part + block_cols
    found_ref[:common, :] = found[:common].astype(jnp.bfloat16)
    found_ref[common:, :] = pack(found[common:, slot_count:]).astype(jnp.bfloat16)
    for copy in outs:
        copy.wait()


def select(pivots, vectors, integrals, slot_count, part):
    panels, block_cols, row_count = integrals.shape
    rows = part + block_cols + block_cols // 2
    outs = [jax.ShapeDtypeStruct((rows, panels * slot_count), jnp.bfloat16)]
    outs += [jax.ShapeDtypeStruct((block_cols, row_count), jnp.bfloat16)] * panels
    results = pl.pallas_call(
        functools.partial(select_kernel, slot_count),
        out_shape=outs,
        in_specs=[pl.BlockSpec(memory_space=pl.ANY)] * 3,
        out_specs=[pl.BlockSpec(memory_space=pltpu.VMEM)]
        + [pl.BlockSpec(memory_space=pltpu.HBM)] * panels,
        scratch_shapes=[
            pltpu.VMEM((part, row_count), jnp.bfloat16),
            pltpu.VMEM(integrals.shape, jnp.bfloat16),
            pltpu.VMEM(pivots.shape, jnp.int32),
            pltpu.SemaphoreType.DMA((row_count // min(SELECT, row_count) + 2 + panels,)),
        ],
        compiler_params=pltpu.CompilerParams(vmem_limit_bytes=ALMOST_ALL),
        cost_estimate=pl.CostEstimate(flops=MICRO * 2, bytes_accessed=3 * MIB, transcendentals=0),
        name="select",
    )(pivots, vectors, integrals)
    return results[0], results[1:]


def places_kernel(weights, slot_count, row_count, pivots_ref, out_ref):
    panels, width = pivots_ref.shape
    lanes = panels * slot_count
    shift = row_count.bit_length() - 1
    me = lax.axis_index("rows")
    square = (width, width)
    places = []
    for panel in range(panels):
        owner = lax.shift_right_logical(
            pivots_ref[panel : panel + 1, :], jnp.full((1, width), shift, jnp.int32)
        )
        floats = owner.astype(jnp.float32)
        same = jnp.broadcast_to(floats, square) == as_column(floats)
        earlier = iota(square, 0) < iota(square, 1)
        rank = jnp.sum(
            jnp.where(same & earlier, 1.0, 0.0), axis=0, keepdims=True
        ).astype(jnp.int32)
        apart = owner ^ me
        block = jnp.zeros_like(owner)
        for mask, weight in weights:
            block = block + jnp.where((apart & mask) != 0, weight, 0)
        places.append(block * lanes + rank)
    out_ref[0:1, :] = jnp.concatenate([places[0], places[1] + slot_count], 1)
    out_ref[1:2, :] = jnp.concatenate([places[1], places[1] + slot_count], 1)


def places_of(pivots, weights, slot_count, row_count):
    return pl.pallas_call(
        functools.partial(places_kernel, weights, slot_count, row_count),
        out_shape=jax.ShapeDtypeStruct((2, 2 * pivots.shape[1]), jnp.int32),
        in_specs=[pl.BlockSpec(memory_space=pltpu.VMEM)],
        out_specs=pl.BlockSpec(memory_space=pltpu.VMEM),
        compiler_params=pltpu.CompilerParams(vmem_limit_bytes=16 * MIB),
        cost_estimate=pl.CostEstimate(flops=MICRO, bytes_accessed=MIB, transcendentals=0),
        name="places",
    )(pivots)


def compact_kernel(places_ref, *refs):
    pieces, outs = refs[:-2], refs[-2:]
    depth, rows, lanes = pieces[0].shape
    common, width = outs[0].shape
    both, halves = places_ref[0:1, :], places_ref[1:2, :]
    main = jnp.zeros((common, 2 * width), jnp.float32)
    rest = jnp.zeros((rows - common, 2 * width), jnp.float32)
    for i in range(len(pieces) * depth):
        lane = iota((lanes, 2 * width), 0) + i * lanes
        x = pieces[i // depth][i % depth]
        main = main + dot(x[:common], jnp.where(lane == both, 1.0, 0.0).astype(jnp.bfloat16))
        rest = rest + dot(x[common:], jnp.where(lane == halves, 1.0, 0.0).astype(jnp.bfloat16))
    outs[0][...] = main[:, :width].astype(jnp.bfloat16)
    outs[1][:common, :] = main[:, width:].astype(jnp.bfloat16)
    outs[1][common:rows, :] = rest[:, :width].astype(jnp.bfloat16)
    outs[1][rows:, :] = rest[:, width:].astype(jnp.bfloat16)


def compact(places, pieces, part):
    rows = pieces[0].shape[1]
    width = places.shape[1] // 2
    block_cols = (rows - part) * 2 // 3
    return pl.pallas_call(
        compact_kernel,
        out_shape=[
            jax.ShapeDtypeStruct((part + block_cols, width), jnp.bfloat16),
            jax.ShapeDtypeStruct((part + 2 * block_cols, width), jnp.bfloat16),
        ],
        in_specs=[pl.BlockSpec(memory_space=pltpu.VMEM)] * (1 + len(pieces)),
        out_specs=[pl.BlockSpec(memory_space=pltpu.VMEM)] * 2,
        compiler_params=pltpu.CompilerParams(vmem_limit_bytes=16 * MIB),
        cost_estimate=pl.CostEstimate(flops=MICRO, bytes_accessed=MIB, transcendentals=0),
        name="compact",
    )(places, *pieces)


def eliminate(block, columns, offset):
    vregs = LEAF // 8
    tiles = {g: [x[8 * v : 8 * v + 8] for v in range(vregs)] for g, x in block.items()}
    sublane = iota((8, LANES), 0)
    pivots = [jnp.zeros((8, LANES), jnp.float32) for _ in range(vregs)]
    for sub in range(0, LEAF, SUB):
        first = sub // 8
        diagonal = tiles[columns][first:]
        cols = [
            [
                jnp.broadcast_to(x[:, offset + sub + k : offset + sub + k + 1], (8, LANES))
                for x in diagonal
            ]
            for k in range(SUB)
        ]
        for j in range(SUB):
            jv, jr = j // 8, j % 8
            live = range(jv, len(diagonal))
            pivot = jnp.broadcast_to(cols[j][jv][jr : jr + 1, :], (8, LANES))
            inverse = 1.0 / pivot
            factor = {v: cols[j][v] * inverse for v in live}
            factor[jv] = jnp.where(sublane > jr, factor[jv], 0.0)
            pivots[first + jv] = jnp.where(sublane == jr, pivot, pivots[first + jv])
            for k in range(j + 1, SUB):
                entry = jnp.broadcast_to(cols[j][k // 8][k % 8 : k % 8 + 1, :], (8, LANES))
                for v in range(k // 8, len(diagonal)):
                    cols[k][v] = cols[k][v] - factor[v] * entry
            for rows in tiles.values():
                entry = jnp.broadcast_to(rows[first + jv][jr : jr + 1, :], (8, LANES))
                for v in live:
                    rows[first + v] = rows[first + v] - factor[v] * entry
    scale = [lax.rsqrt(pivot) for pivot in pivots]
    return {
        g: jnp.concatenate([x * y for x, y in zip(rows, scale)], 0) for g, rows in tiles.items()
    }


def start_factor(matrix, work):
    width = matrix.shape[0]
    square = (width, width)
    work[:, :width] = 0.5 * (matrix + matrix.T)
    work[:, width:] = jnp.where(iota(square, 0) == iota(square, 1), 1.0, 0.0)


def lanes_of(g):
    return slice(g * LANES, (g + 1) * LANES)


def run_leaves(work, begin, end):
    width = work.shape[0]
    half = width // LANES
    block = None
    for start in range(begin, end, LEAF):
        following = start + LEAF
        rights = [half + g for g in range((following - 1) // LANES + 1)]
        groups = list(range(start // LANES, half)) + rights
        if block is None:
            block = {g: work[start:following, lanes_of(g)] for g in groups}
        upper = eliminate(block, start // LANES, start % LANES)
        for g in rights:
            work[start:following, lanes_of(g)] = upper[g]
        if following == width:
            break
        lefts = list(range(following // LANES, half))
        used = lefts + rights
        base = lefts[0] * LANES
        high, low = split(jnp.concatenate([upper[g] for g in used], 1))
        right = jnp.concatenate([high, high, low], 0)

        def product(first, last):
            a = high[:, first - base : last - base]
            b = low[:, first - base : last - base]
            return dot(jnp.concatenate([a, b, a], 0), right, 0, 0)

        stop = following + LEAF
        change = product(following, stop)
        block = {}
        for g in lefts + [half + g for g in range((stop - 1) // LANES + 1)]:
            block[g] = work[following:stop, lanes_of(g)]
            if g in used:
                block[g] = block[g] - change[:, lanes_of(used.index(g))]
        if following == end:
            for g, x in block.items():
                work[following:stop, lanes_of(g)] = x
        if stop < width:
            change = product(stop, width)
            for i, g in enumerate(used):
                work[stop:, lanes_of(g)] = work[stop:, lanes_of(g)] - change[:, lanes_of(i)]


def first_kernel(apart, part, *refs):
    count = len(apart)
    picked = refs[:count]
    work, rows_of, ints = refs[count:]
    me = lax.axis_index("cols")
    block_cols = picked[0].shape[0] - part
    for ref, bits in zip(picked, apart):
        at = pl.multiple_of((me ^ bits) * block_cols, block_cols)
        rows_of[pl.ds(pl.multiple_of((me ^ bits) * part, part), part), :] = ref[:part, :]
        ints[pl.ds(at, block_cols), :] = ref[part:, :].astype(jnp.float32)
    at_pivots = rows_of[...]
    start_factor(ints[...] - dot(at_pivots, at_pivots, 0, 0), work)
    run_leaves(work, 0, work.shape[0] // 2)


def first_half(picked, apart, part):
    count = len(apart)
    _, width = picked[0].shape
    return pl.pallas_call(
        functools.partial(first_kernel, apart, part),
        out_shape=jax.ShapeDtypeStruct((width, 2 * width), jnp.float32),
        in_specs=[pl.BlockSpec(memory_space=pltpu.VMEM)] * count,
        out_specs=pl.BlockSpec(memory_space=pltpu.VMEM),
        scratch_shapes=[
            pltpu.VMEM((count * part, width), jnp.bfloat16),
            pltpu.VMEM((width, width), jnp.float32),
        ],
        compiler_params=pltpu.CompilerParams(vmem_limit_bytes=16 * MIB),
        cost_estimate=pl.CostEstimate(flops=4 * MICRO, bytes_accessed=MIB, transcendentals=0),
        name="first_half",
    )(*picked)


def second_kernel(before_ref, work):
    work[...] = before_ref[...]
    run_leaves(work, work.shape[0] // 2, work.shape[0])


def second_half(work):
    return pl.pallas_call(
        second_kernel,
        out_shape=jax.ShapeDtypeStruct(work.shape, work.dtype),
        in_specs=[pl.BlockSpec(memory_space=pltpu.VMEM)],
        out_specs=pl.BlockSpec(memory_space=pltpu.VMEM),
        compiler_params=pltpu.CompilerParams(vmem_limit_bytes=16 * MIB),
        cost_estimate=pl.CostEstimate(flops=4 * MICRO, bytes_accessed=MIB, transcendentals=0),
        name="second_half",
    )(work)


def third_kernel(apart, part, *refs):
    count = len(apart)
    work0, picked0, picked1 = refs[0], refs[1 : 1 + count], refs[1 + count : 1 + 2 * count]
    work1, rows_of, ahead_ref, ints0, ints1 = refs[1 + 2 * count :]
    me = lax.axis_index("cols")
    width = work0.shape[0]
    block_cols = picked0[0].shape[0] - part
    for i, bits in enumerate(apart):
        at = pl.ds(pl.multiple_of((me ^ bits) * part, part), part)
        rows_of[at, :width] = picked0[i][:part, :]
        rows_of[at, width:] = picked1[i][:part, :]
        at = pl.ds(pl.multiple_of((me ^ bits) * block_cols, block_cols), block_cols)
        ints0[at, :] = picked1[i][part : part + block_cols, :].astype(jnp.float32)
        ints1[at, :] = picked1[i][part + block_cols :, :].astype(jnp.float32)
    gram = dot(rows_of[...], rows_of[:, width:], 0, 0)
    ahead = product_wide(work0[:, width:], ints0[...] - gram[:width]).astype(jnp.bfloat16)
    ahead_ref[...] = ahead
    start_factor(ints1[...] - gram[width:] - dot(ahead, ahead, 0, 0), work1)
    run_leaves(work1, 0, width // 2)


def third_half(work0, picked0, picked1, apart, part):
    count = len(apart)
    width = work0.shape[0]
    return pl.pallas_call(
        functools.partial(third_kernel, apart, part),
        out_shape=[
            jax.ShapeDtypeStruct(work0.shape, jnp.float32),
            jax.ShapeDtypeStruct((count * part, 2 * width), jnp.bfloat16),
            jax.ShapeDtypeStruct((width, width), jnp.bfloat16),
        ],
        in_specs=[pl.BlockSpec(memory_space=pltpu.VMEM)] * (1 + 2 * count),
        out_specs=[pl.BlockSpec(memory_space=pltpu.VMEM)] * 3,
        scratch_shapes=[pltpu.VMEM((width, width), jnp.float32)] * 2,
        compiler_params=pltpu.CompilerParams(vmem_limit_bytes=16 * MIB),
        cost_estimate=pl.CostEstimate(flops=5 * MICRO, bytes_accessed=MIB, transcendentals=0),
        name="third_half",
    )(work0, *picked0, *picked1)


def fourth_kernel(apart, block_cols, work0, before_ref, rows_of, ahead, left, work1):
    width = work0.shape[0]
    both = 2 * width
    work1[...] = before_ref[...]
    run_leaves(work1, width // 2, width)
    me = lax.axis_index("cols")
    mine = pl.ds(pl.multiple_of(me * block_cols, block_cols), block_cols)
    inverse0 = work0[mine, width:]
    inverse1 = work1[mine, width:]
    through = product_wide(product_narrow(inverse1, ahead[...], 1), work0[:, width:])
    small = jnp.concatenate(
        [
            jnp.concatenate([inverse0, jnp.zeros_like(inverse0)], 1),
            jnp.concatenate([-through, inverse1], 1),
        ],
        0,
    )
    ordered = []
    for panel in range(2):
        for bits in apart:
            source = me ^ bits
            piece = jnp.zeros((2 * block_cols, block_cols), jnp.float32)
            for block in range(len(apart)):
                at = panel * width + block * block_cols
                piece = jnp.where(source == block, small[:, at : at + block_cols], piece)
            ordered.append(piece)
    left[:, :both] = jnp.concatenate(split(jnp.concatenate(ordered, 1)), 0)
    left[:, both:] = jnp.concatenate(split(-product_narrow(small, rows_of[...], 1)), 0)


def fourth_half(work0, work1, rows_of, ahead, apart, block_cols):
    width = work0.shape[0]
    return pl.pallas_call(
        functools.partial(fourth_kernel, apart, block_cols),
        out_shape=jax.ShapeDtypeStruct(
            (4 * block_cols, 2 * width + rows_of.shape[0]), jnp.bfloat16
        ),
        in_specs=[pl.BlockSpec(memory_space=pltpu.VMEM)] * 4,
        out_specs=pl.BlockSpec(memory_space=pltpu.VMEM),
        scratch_shapes=[pltpu.VMEM(work0.shape, jnp.float32)],
        compiler_params=pltpu.CompilerParams(vmem_limit_bytes=16 * MIB),
        cost_estimate=pl.CostEstimate(flops=5 * MICRO, bytes_accessed=MIB, transcendentals=0),
        name="fourth_half",
    )(work0, work1, rows_of, ahead)


def finish_kernel(left, vectors_ref, *refs):
    blocks, (out_ref, result, out_sems) = refs[:-3], refs[-3:]
    pairs = vectors_ref.shape[1]
    block_cols = blocks[0].shape[0]
    both = len(blocks) * block_cols
    outs = []
    for n in range(pairs // CHUNK):
        at = slice(n * CHUNK, (n + 1) * CHUNK)
        right = jnp.concatenate([ref[:, at] for ref in blocks], 0)
        halves = dot(left[:, both:], vectors_ref[:, at]) + dot(left[:, :both], right)
        value = halves[: 2 * block_cols] + halves[2 * block_cols :]
        result[0, :, at] = value[:block_cols]
        result[1, :, at] = value[block_cols:]
        outs.append(
            pltpu.make_async_copy(result.at[:, :, at], out_ref.at[:, :, at], out_sems.at[n])
        )
        outs[-1].start()
    for copy in outs:
        copy.wait()


def finish(left, vectors, blocks):
    block_cols, pairs = blocks[0].shape
    return pl.pallas_call(
        finish_kernel,
        out_shape=jax.ShapeDtypeStruct((2, block_cols, pairs), jnp.float32),
        in_specs=[pl.BlockSpec(memory_space=pltpu.VMEM)] * (2 + len(blocks)),
        out_specs=pl.BlockSpec(memory_space=pl.ANY),
        scratch_shapes=[
            pltpu.VMEM((2, block_cols, pairs), jnp.float32),
            pltpu.SemaphoreType.DMA((pairs // CHUNK,)),
        ],
        compiler_params=pltpu.CompilerParams(vmem_limit_bytes=24 * MIB),
        cost_estimate=pl.CostEstimate(
            flops=6 * MICRO, bytes_accessed=16 * MIB, transcendentals=0
        ),
        name="finish",
    )(left, vectors, *blocks)


def per_device(vectors, integrals, pivots):
    prior, row_count = vectors.shape
    _, width = pivots.shape
    owners, col_count = lax.axis_size("rows"), lax.axis_size("cols")
    block_cols = integrals.shape[1]
    slot_count = 2 * width // owners
    part = prior // col_count

    def swap(x, axis, mask):
        size = lax.axis_size(axis)
        return lax.ppermute(x, axis, [(i, i ^ mask) for i in range(size)])

    def near(pieces):
        return [swap(piece, "cols", near_mask) for piece in pieces]

    far_mask, near_mask = masks_of(col_count)
    apart = [0, far_mask, near_mask, far_mask ^ near_mask]

    found, ints = select(pivots, vectors, integrals, slot_count, part)
    masks = masks_of(owners)
    held = found[None]
    depth, weights = 1, []
    for mask in masks[:-3]:
        held = jnp.concatenate([held, swap(held, "rows", mask)], 0)
        weights.append((mask, depth))
        depth = 2 * depth
    weights += [(mask, depth << i) for i, mask in enumerate(masks[-3:])]
    passed = swap(held, "rows", masks[-3])
    pieces = [held, passed]
    for mask in (masks[-2], masks[-1], masks[-2] ^ masks[-1]):
        pieces.append(swap(held, "rows", mask))
        pieces.append(swap(passed, "rows", mask))
    places = places_of(pivots, weights, slot_count, row_count)
    own0, own1 = compact(places, pieces, part)

    far0 = swap(ints[0], "cols", far_mask)
    other0 = swap(own0, "cols", far_mask)
    other1 = swap(own1, "cols", far_mask)
    picked0 = [own0, other0] + near([own0]) + near([other0])
    beside1 = near([own1])
    beside = near(ints)
    far1 = swap(ints[1], "cols", far_mask)
    work0 = first_half(picked0, apart, part)
    work0, other1, far0 = lax.optimization_barrier((work0, other1, far0))
    picked1 = [own1, other1] + beside1 + near([other1])
    blocks = [ints[0], far0, beside[0]] + near([far0])
    work0 = second_half(work0)
    work1, rows_of, ahead = third_half(work0, picked0, picked1, apart, part)
    work1, far1 = lax.optimization_barrier((work1, far1))
    blocks += [ints[1], far1, beside[1]] + near([far1])
    left = fourth_half(work0, work1, rows_of, ahead, apart, block_cols)
    return finish(left, vectors, blocks)


def solution(mesh):
    placed = (P(None, "rows"), P(None, "cols", "rows"), P())

    return jax.shard_map(
        per_device, mesh=mesh, in_specs=placed, out_specs=P(None, "cols", "rows"), check_vma=False
    )
```

```python
import functools

import jax
import jax.numpy as jnp
from jax import lax
from jax.experimental import pallas as pl
from jax.experimental.pallas import tpu as pltpu
from jax.sharding import PartitionSpec as P

LANES = 128
LEAF = 32
SUB = 16
CHUNK = 512
SELECT = 512
MICRO = 1 << 29
MIB = 1 << 20
ALMOST_ALL = 52 * MIB


def masks_of(size):
    return [1 << bit for bit in reversed(range(size.bit_length() - 1))]


def dot(left, right, left_dim=1, right_dim=0):
    return lax.dot_general(
        left, right, (((left_dim,), (right_dim,)), ((), ())), preferred_element_type=jnp.float32
    )


def split(x):
    high = x.astype(jnp.bfloat16)
    return high, (x - high.astype(jnp.float32)).astype(jnp.bfloat16)


def product_narrow(left, right, right_dim=0):
    rows = left.shape[0]
    both = dot(jnp.concatenate(split(left), 0), right, 1, right_dim)
    return both[:rows] + both[rows:]


def product_wide(left, right):
    left_high, left_low = split(left)
    right_high, right_low = split(right)
    return dot(
        jnp.concatenate([left_high, left_low, left_high], 1),
        jnp.concatenate([right_high, right_high, right_low], 0),
    )


def iota(shape, dim):
    return lax.broadcasted_iota(jnp.int32, shape, dim)


def as_column(row):
    size = row.shape[1]
    square = (size, size)
    return jnp.sum(
        jnp.where(iota(square, 0) == iota(square, 1), jnp.broadcast_to(row, square), 0.0),
        axis=1,
        keepdims=True,
    )


def pack(x):
    half = x.shape[0] // 2
    return jnp.concatenate([x[:half], x[half:]], 1)


def select_kernel(slot_count, pivots_ref, vectors_ref, integrals_ref, *refs):
    panels, block_cols, _ = integrals_ref.shape
    found_ref, out_refs = refs[0], refs[1 : 1 + panels]
    vec, ints, local_pivots, sems = refs[1 + panels :]
    part, row_count = vec.shape
    width = pivots_ref.shape[1]
    listed = pltpu.make_async_copy(pivots_ref, local_pivots, sems.at[sems.shape[0] - 1])
    listed.start()
    lanes = panels * slot_count
    first = pl.multiple_of(lax.axis_index("cols") * part, part)
    step = min(SELECT, row_count)
    count = row_count // step
    copies = []
    for n in range(count):
        at = pl.ds(n * step, step)
        copies.append(
            pltpu.make_async_copy(
                vectors_ref.at[pl.ds(first, part), at], vec.at[:, at], sems.at[n]
            )
        )
    whole = pltpu.make_async_copy(integrals_ref, ints, sems.at[count])
    for copy in copies[:1] + [whole] + copies[1:]:
        copy.start()
    listed.wait()
    start = (lax.axis_index("rows") * row_count).astype(jnp.float32)
    square = (width, width)
    target = jnp.zeros((1, lanes), jnp.float32)
    for panel in range(panels):
        local = local_pivots[panel : panel + 1, :].astype(jnp.float32) - start
        mine = ((local >= 0.0) & (local < row_count)).astype(jnp.float32)
        earlier = iota(square, 1) < iota(square, 0)
        rank = jnp.sum(
            jnp.where(earlier, jnp.broadcast_to(mine, square), 0.0), axis=1, keepdims=True
        )
        held = as_column(jnp.where(mine > 0.0, local + 1.0, 0.0))
        slot = iota((width, lanes), 1).astype(jnp.float32) - panel * slot_count
        target = target + jnp.sum(jnp.where(rank == slot, held, 0.0), axis=0, keepdims=True)
    target = target.astype(jnp.int32) - 1
    whole.wait()
    outs = [
        pltpu.make_async_copy(ints.at[panel], out_refs[panel], sems.at[count + 1 + panel])
        for panel in range(panels)
    ]
    for copy in outs:
        copy.start()
    found = jnp.zeros((part + panels * block_cols, lanes), jnp.float32)
    for n, copy in enumerate(copies):
        copy.wait()
        at = slice(n * step, (n + 1) * step)
        pick = jnp.where(iota((step, lanes), 0) + n * step == target, 1.0, 0.0).astype(jnp.bfloat16)
        left = jnp.concatenate([vec[:, at]] + [ints[panel, :, at] for panel in range(panels)], 0)
        found = found + dot(left, pick)
    common = part + block_cols
    found_ref[:common, :] = found[:common].astype(jnp.bfloat16)
    found_ref[common:, :] = pack(found[common:, slot_count:]).astype(jnp.bfloat16)
    for copy in outs:
        copy.wait()


def select(pivots, vectors, integrals, slot_count, part):
    panels, block_cols, row_count = integrals.shape
    rows = part + block_cols + block_cols // 2
    outs = [jax.ShapeDtypeStruct((rows, panels * slot_count), jnp.bfloat16)]
    outs += [jax.ShapeDtypeStruct((block_cols, row_count), jnp.bfloat16)] * panels
    results = pl.pallas_call(
        functools.partial(select_kernel, slot_count),
        out_shape=outs,
        in_specs=[pl.BlockSpec(memory_space=pl.ANY)] * 3,
        out_specs=[pl.BlockSpec(memory_space=pltpu.VMEM)]
        + [pl.BlockSpec(memory_space=pltpu.HBM)] * panels,
        scratch_shapes=[
            pltpu.VMEM((part, row_count), jnp.bfloat16),
            pltpu.VMEM(integrals.shape, jnp.bfloat16),
            pltpu.VMEM(pivots.shape, jnp.int32),
            pltpu.SemaphoreType.DMA((row_count // min(SELECT, row_count) + 2 + panels,)),
        ],
        compiler_params=pltpu.CompilerParams(vmem_limit_bytes=ALMOST_ALL),
        cost_estimate=pl.CostEstimate(flops=MICRO * 2, bytes_accessed=3 * MIB, transcendentals=0),
        name="select",
    )(pivots, vectors, integrals)
    return results[0], results[1:]


def places_kernel(weights, slot_count, row_count, pivots_ref, out_ref):
    panels, width = pivots_ref.shape
    lanes = panels * slot_count
    shift = row_count.bit_length() - 1
    me = lax.axis_index("rows")
    square = (width, width)
    places = []
    for panel in range(panels):
        owner = lax.shift_right_logical(
            pivots_ref[panel : panel + 1, :], jnp.full((1, width), shift, jnp.int32)
        )
        floats = owner.astype(jnp.float32)
        same = jnp.broadcast_to(floats, square) == as_column(floats)
        earlier = iota(square, 0) < iota(square, 1)
        rank = jnp.sum(
            jnp.where(same & earlier, 1.0, 0.0), axis=0, keepdims=True
        ).astype(jnp.int32)
        apart = owner ^ me
        block = jnp.zeros_like(owner)
        for mask, weight in weights:
            block = block + jnp.where((apart & mask) != 0, weight, 0)
        places.append(block * lanes + rank)
    out_ref[0:1, :] = jnp.concatenate([places[0], places[1] + slot_count], 1)
    out_ref[1:2, :] = jnp.concatenate([places[1], places[1] + slot_count], 1)


def places_of(pivots, weights, slot_count, row_count):
    return pl.pallas_call(
        functools.partial(places_kernel, weights, slot_count, row_count),
        out_shape=jax.ShapeDtypeStruct((2, 2 * pivots.shape[1]), jnp.int32),
        in_specs=[pl.BlockSpec(memory_space=pltpu.VMEM)],
        out_specs=pl.BlockSpec(memory_space=pltpu.VMEM),
        compiler_params=pltpu.CompilerParams(vmem_limit_bytes=16 * MIB),
        cost_estimate=pl.CostEstimate(flops=MICRO, bytes_accessed=MIB, transcendentals=0),
        name="places",
    )(pivots)


def compact_kernel(places_ref, *refs):
    pieces, outs = refs[:-2], refs[-2:]
    depth, rows, lanes = pieces[0].shape
    common, width = outs[0].shape
    both, halves = places_ref[0:1, :], places_ref[1:2, :]
    main = jnp.zeros((common, 2 * width), jnp.float32)
    rest = jnp.zeros((rows - common, 2 * width), jnp.float32)
    for i in range(len(pieces) * depth):
        lane = iota((lanes, 2 * width), 0) + i * lanes
        x = pieces[i // depth][i % depth]
        main = main + dot(x[:common], jnp.where(lane == both, 1.0, 0.0).astype(jnp.bfloat16))
        rest = rest + dot(x[common:], jnp.where(lane == halves, 1.0, 0.0).astype(jnp.bfloat16))
    outs[0][...] = main[:, :width].astype(jnp.bfloat16)
    outs[1][:common, :] = main[:, width:].astype(jnp.bfloat16)
    outs[1][common:rows, :] = rest[:, :width].astype(jnp.bfloat16)
    outs[1][rows:, :] = rest[:, width:].astype(jnp.bfloat16)


def compact(places, pieces, part):
    rows = pieces[0].shape[1]
    width = places.shape[1] // 2
    block_cols = (rows - part) * 2 // 3
    return pl.pallas_call(
        compact_kernel,
        out_shape=[
            jax.ShapeDtypeStruct((part + block_cols, width), jnp.bfloat16),
            jax.ShapeDtypeStruct((part + 2 * block_cols, width), jnp.bfloat16),
        ],
        in_specs=[pl.BlockSpec(memory_space=pltpu.VMEM)] * (1 + len(pieces)),
        out_specs=[pl.BlockSpec(memory_space=pltpu.VMEM)] * 2,
        compiler_params=pltpu.CompilerParams(vmem_limit_bytes=16 * MIB),
        cost_estimate=pl.CostEstimate(flops=MICRO, bytes_accessed=MIB, transcendentals=0),
        name="compact",
    )(places, *pieces)


def eliminate(block, columns, offset):
    vregs = LEAF // 8
    tiles = {g: [x[8 * v : 8 * v + 8] for v in range(vregs)] for g, x in block.items()}
    sublane = iota((8, LANES), 0)
    pivots = [jnp.zeros((8, LANES), jnp.float32) for _ in range(vregs)]
    for sub in range(0, LEAF, SUB):
        first = sub // 8
        diagonal = tiles[columns][first:]
        cols = [
            [
                jnp.broadcast_to(x[:, offset + sub + k : offset + sub + k + 1], (8, LANES))
                for x in diagonal
            ]
            for k in range(SUB)
        ]
        for j in range(SUB):
            jv, jr = j // 8, j % 8
            live = range(jv, len(diagonal))
            pivot = jnp.broadcast_to(cols[j][jv][jr : jr + 1, :], (8, LANES))
            inverse = 1.0 / pivot
            factor = {v: cols[j][v] * inverse for v in live}
            factor[jv] = jnp.where(sublane > jr, factor[jv], 0.0)
            pivots[first + jv] = jnp.where(sublane == jr, pivot, pivots[first + jv])
            for k in range(j + 1, SUB):
                entry = jnp.broadcast_to(cols[j][k // 8][k % 8 : k % 8 + 1, :], (8, LANES))
                for v in range(k // 8, len(diagonal)):
                    cols[k][v] = cols[k][v] - factor[v] * entry
            for rows in tiles.values():
                entry = jnp.broadcast_to(rows[first + jv][jr : jr + 1, :], (8, LANES))
                for v in live:
                    rows[first + v] = rows[first + v] - factor[v] * entry
    scale = [lax.rsqrt(pivot) for pivot in pivots]
    return {
        g: jnp.concatenate([x * y for x, y in zip(rows, scale)], 0) for g, rows in tiles.items()
    }


def start_factor(matrix, work):
    width = matrix.shape[0]
    square = (width, width)
    work[:, :width] = 0.5 * (matrix + matrix.T)
    work[:, width:] = jnp.where(iota(square, 0) == iota(square, 1), 1.0, 0.0)


def lanes_of(g):
    return slice(g * LANES, (g + 1) * LANES)


def run_leaves(work, begin, end):
    width = work.shape[0]
    half = width // LANES
    block = None
    for start in range(begin, end, LEAF):
        following = start + LEAF
        rights = [half + g for g in range((following - 1) // LANES + 1)]
        groups = list(range(start // LANES, half)) + rights
        if block is None:
            block = {g: work[start:following, lanes_of(g)] for g in groups}
        upper = eliminate(block, start // LANES, start % LANES)
        for g in rights:
            work[start:following, lanes_of(g)] = upper[g]
        if following == width:
            break
        lefts = list(range(following // LANES, half))
        used = lefts + rights
        base = lefts[0] * LANES
        high, low = split(jnp.concatenate([upper[g] for g in used], 1))
        right = jnp.concatenate([high, high, low], 0)

        def product(first, last):
            a = high[:, first - base : last - base]
            b = low[:, first - base : last - base]
            return dot(jnp.concatenate([a, b, a], 0), right, 0, 0)

        stop = following + LEAF
        change = product(following, stop)
        block = {}
        for g in lefts + [half + g for g in range((stop - 1) // LANES + 1)]:
            block[g] = work[following:stop, lanes_of(g)]
            if g in used:
                block[g] = block[g] - change[:, lanes_of(used.index(g))]
        if following == end:
            for g, x in block.items():
                work[following:stop, lanes_of(g)] = x
        if stop < width:
            change = product(stop, width)
            for i, g in enumerate(used):
                work[stop:, lanes_of(g)] = work[stop:, lanes_of(g)] - change[:, lanes_of(i)]


def first_kernel(apart, part, *refs):
    count = len(apart)
    picked = refs[:count]
    work, rows_of, ints = refs[count:]
    me = lax.axis_index("cols")
    block_cols = picked[0].shape[0] - part
    for ref, bits in zip(picked, apart):
        at = pl.multiple_of((me ^ bits) * block_cols, block_cols)
        rows_of[pl.ds(pl.multiple_of((me ^ bits) * part, part), part), :] = ref[:part, :]
        ints[pl.ds(at, block_cols), :] = ref[part:, :].astype(jnp.float32)
    at_pivots = rows_of[...]
    start_factor(ints[...] - dot(at_pivots, at_pivots, 0, 0), work)
    run_leaves(work, 0, work.shape[0] // 2)


def first_half(picked, apart, part):
    count = len(apart)
    _, width = picked[0].shape
    return pl.pallas_call(
        functools.partial(first_kernel, apart, part),
        out_shape=jax.ShapeDtypeStruct((width, 2 * width), jnp.float32),
        in_specs=[pl.BlockSpec(memory_space=pltpu.VMEM)] * count,
        out_specs=pl.BlockSpec(memory_space=pltpu.VMEM),
        scratch_shapes=[
            pltpu.VMEM((count * part, width), jnp.bfloat16),
            pltpu.VMEM((width, width), jnp.float32),
        ],
        compiler_params=pltpu.CompilerParams(vmem_limit_bytes=16 * MIB),
        cost_estimate=pl.CostEstimate(flops=4 * MICRO, bytes_accessed=MIB, transcendentals=0),
        name="first_half",
    )(*picked)


def second_kernel(before_ref, work):
    work[...] = before_ref[...]
    run_leaves(work, work.shape[0] // 2, work.shape[0])


def second_half(work):
    return pl.pallas_call(
        second_kernel,
        out_shape=jax.ShapeDtypeStruct(work.shape, work.dtype),
        in_specs=[pl.BlockSpec(memory_space=pltpu.VMEM)],
        out_specs=pl.BlockSpec(memory_space=pltpu.VMEM),
        compiler_params=pltpu.CompilerParams(vmem_limit_bytes=16 * MIB),
        cost_estimate=pl.CostEstimate(flops=4 * MICRO, bytes_accessed=MIB, transcendentals=0),
        name="second_half",
    )(work)


def third_kernel(apart, part, *refs):
    count = len(apart)
    work0, picked0, picked1 = refs[0], refs[1 : 1 + count], refs[1 + count : 1 + 2 * count]
    work1, rows_of, ahead_ref, ints0, ints1 = refs[1 + 2 * count :]
    me = lax.axis_index("cols")
    width = work0.shape[0]
    block_cols = picked0[0].shape[0] - part
    for i, bits in enumerate(apart):
        at = pl.ds(pl.multiple_of((me ^ bits) * part, part), part)
        rows_of[at, :width] = picked0[i][:part, :]
        rows_of[at, width:] = picked1[i][:part, :]
        at = pl.ds(pl.multiple_of((me ^ bits) * block_cols, block_cols), block_cols)
        ints0[at, :] = picked1[i][part : part + block_cols, :].astype(jnp.float32)
        ints1[at, :] = picked1[i][part + block_cols :, :].astype(jnp.float32)
    gram = dot(rows_of[...], rows_of[:, width:], 0, 0)
    ahead = product_wide(work0[:, width:], ints0[...] - gram[:width]).astype(jnp.bfloat16)
    ahead_ref[...] = ahead
    start_factor(ints1[...] - gram[width:] - dot(ahead, ahead, 0, 0), work1)
    run_leaves(work1, 0, width // 2)


def third_half(work0, picked0, picked1, apart, part):
    count = len(apart)
    width = work0.shape[0]
    return pl.pallas_call(
        functools.partial(third_kernel, apart, part),
        out_shape=[
            jax.ShapeDtypeStruct(work0.shape, jnp.float32),
            jax.ShapeDtypeStruct((count * part, 2 * width), jnp.bfloat16),
            jax.ShapeDtypeStruct((width, width), jnp.bfloat16),
        ],
        in_specs=[pl.BlockSpec(memory_space=pltpu.VMEM)] * (1 + 2 * count),
        out_specs=[pl.BlockSpec(memory_space=pltpu.VMEM)] * 3,
        scratch_shapes=[pltpu.VMEM((width, width), jnp.float32)] * 2,
        compiler_params=pltpu.CompilerParams(vmem_limit_bytes=16 * MIB),
        cost_estimate=pl.CostEstimate(flops=5 * MICRO, bytes_accessed=MIB, transcendentals=0),
        name="third_half",
    )(work0, *picked0, *picked1)


def fourth_kernel(apart, block_cols, work0, before_ref, rows_of, ahead, left, work1):
    width = work0.shape[0]
    square = (width, width)
    me = lax.axis_index("cols")
    mine = pl.ds(pl.multiple_of(me * block_cols, block_cols), block_cols)
    work1[...] = before_ref[...]
    lane = iota(square, 1)
    source = iota(square, 0)
    arrive = jnp.zeros(square, jnp.float32)
    for i, bits in enumerate(apart):
        shifted = lane + ((me ^ bits) - i) * block_cols
        here = (lane >= i * block_cols) & (lane < (i + 1) * block_cols)
        arrive = jnp.where(here & (source == shifted), 1.0, arrive)
    arrive = arrive.astype(jnp.bfloat16)
    same = jnp.where(source == lane, 1.0, 0.0).astype(jnp.bfloat16)
    inverse_high, inverse_low = split(work0[:, width:])
    through = dot(ahead[...], inverse_high, 0, 0) + dot(ahead[...], inverse_low, 0, 0)
    through_high, through_low = split(through)
    early, late = rows_of[:, :width], rows_of[:, width:]
    on_vectors = dot(
        jnp.concatenate([same, -through_high, -through_low], 1),
        jnp.concatenate([late, early, early], 1),
        1,
        1,
    )
    right_high, right_low = split(
        jnp.concatenate([-product_narrow(through, arrive), -on_vectors], 1)
    )
    right_high = jnp.concatenate([right_high[:, :width], arrive, right_high[:, width:]], 1)
    right_low = jnp.concatenate(
        [right_low[:, :width], jnp.zeros_like(arrive), right_low[:, width:]], 1
    )
    right = jnp.concatenate([right_high, right_high, right_low], 0)
    inverse0 = work0[mine, width:]
    top = jnp.concatenate(
        [
            product_narrow(inverse0, arrive),
            jnp.zeros((block_cols, width), jnp.float32),
            -product_narrow(inverse0, early, 1),
        ],
        1,
    )
    top_high, top_low = split(top)
    left[:block_cols, :] = top_high
    left[2 * block_cols : 3 * block_cols, :] = top_low

    run_leaves(work1, width // 2, width)
    high, low = split(work1[mine, width:])
    low_high, low_low = split(dot(jnp.concatenate([high, low, high], 1), right))
    left[block_cols : 2 * block_cols, :] = low_high
    left[3 * block_cols :, :] = low_low


def fourth_half(work0, work1, rows_of, ahead, apart, block_cols):
    width = work0.shape[0]
    return pl.pallas_call(
        functools.partial(fourth_kernel, apart, block_cols),
        out_shape=jax.ShapeDtypeStruct(
            (4 * block_cols, 2 * width + rows_of.shape[0]), jnp.bfloat16
        ),
        in_specs=[pl.BlockSpec(memory_space=pltpu.VMEM)] * 4,
        out_specs=pl.BlockSpec(memory_space=pltpu.VMEM),
        scratch_shapes=[pltpu.VMEM(work0.shape, jnp.float32)],
        compiler_params=pltpu.CompilerParams(vmem_limit_bytes=16 * MIB),
        cost_estimate=pl.CostEstimate(flops=5 * MICRO, bytes_accessed=MIB, transcendentals=0),
        name="fourth_half",
    )(work0, work1, rows_of, ahead)


def finish_kernel(left, vectors_ref, *refs):
    blocks, (out_ref, result, out_sems) = refs[:-3], refs[-3:]
    pairs = vectors_ref.shape[1]
    block_cols = blocks[0].shape[0]
    both = len(blocks) * block_cols
    outs = []
    for n in range(pairs // CHUNK):
        at = slice(n * CHUNK, (n + 1) * CHUNK)
        right = jnp.concatenate([ref[:, at] for ref in blocks], 0)
        halves = dot(left[:, both:], vectors_ref[:, at]) + dot(left[:, :both], right)
        value = halves[: 2 * block_cols] + halves[2 * block_cols :]
        result[0, :, at] = value[:block_cols]
        result[1, :, at] = value[block_cols:]
        outs.append(
            pltpu.make_async_copy(result.at[:, :, at], out_ref.at[:, :, at], out_sems.at[n])
        )
        outs[-1].start()
    for copy in outs:
        copy.wait()


def finish(left, vectors, blocks):
    block_cols, pairs = blocks[0].shape
    return pl.pallas_call(
        finish_kernel,
        out_shape=jax.ShapeDtypeStruct((2, block_cols, pairs), jnp.float32),
        in_specs=[pl.BlockSpec(memory_space=pltpu.VMEM)] * (2 + len(blocks)),
        out_specs=pl.BlockSpec(memory_space=pl.ANY),
        scratch_shapes=[
            pltpu.VMEM((2, block_cols, pairs), jnp.float32),
            pltpu.SemaphoreType.DMA((pairs // CHUNK,)),
        ],
        compiler_params=pltpu.CompilerParams(vmem_limit_bytes=24 * MIB),
        cost_estimate=pl.CostEstimate(
            flops=6 * MICRO, bytes_accessed=16 * MIB, transcendentals=0
        ),
        name="finish",
    )(left, vectors, *blocks)


def per_device(vectors, integrals, pivots):
    prior, row_count = vectors.shape
    _, width = pivots.shape
    owners, col_count = lax.axis_size("rows"), lax.axis_size("cols")
    block_cols = integrals.shape[1]
    slot_count = 2 * width // owners
    part = prior // col_count

    def swap(x, axis, mask):
        size = lax.axis_size(axis)
        return lax.ppermute(x, axis, [(i, i ^ mask) for i in range(size)])

    def near(pieces):
        return [swap(piece, "cols", near_mask) for piece in pieces]

    far_mask, near_mask = masks_of(col_count)
    apart = [0, far_mask, near_mask, far_mask ^ near_mask]

    found, ints = select(pivots, vectors, integrals, slot_count, part)
    masks = masks_of(owners)
    held = found[None]
    depth, weights = 1, []
    for mask in masks[:-3]:
        held = jnp.concatenate([held, swap(held, "rows", mask)], 0)
        weights.append((mask, depth))
        depth = 2 * depth
    weights += [(mask, depth << i) for i, mask in enumerate(masks[-3:])]
    passed = swap(held, "rows", masks[-3])
    pieces = [held, passed]
    for mask in (masks[-2], masks[-1], masks[-2] ^ masks[-1]):
        pieces.append(swap(held, "rows", mask))
        pieces.append(swap(passed, "rows", mask))
    places = places_of(pivots, weights, slot_count, row_count)
    own0, own1 = compact(places, pieces, part)

    far0 = swap(ints[0], "cols", far_mask)
    other0 = swap(own0, "cols", far_mask)
    other1 = swap(own1, "cols", far_mask)
    picked0 = [own0, other0] + near([own0]) + near([other0])
    beside1 = near([own1])
    beside = near(ints)
    far1 = swap(ints[1], "cols", far_mask)
    work0 = first_half(picked0, apart, part)
    work0, other1, far0 = lax.optimization_barrier((work0, other1, far0))
    picked1 = [own1, other1] + beside1 + near([other1])
    blocks = [ints[0], far0, beside[0]] + near([far0])
    work0 = second_half(work0)
    work1, rows_of, ahead = third_half(work0, picked0, picked1, apart, part)
    work1, far1 = lax.optimization_barrier((work1, far1))
    blocks += [ints[1], far1, beside[1]] + near([far1])
    left = fourth_half(work0, work1, rows_of, ahead, apart, block_cols)
    return finish(left, vectors, blocks)


def solution(mesh):
    placed = (P(None, "rows"), P(None, "cols", "rows"), P())

    return jax.shard_map(
        per_device, mesh=mesh, in_specs=placed, out_specs=P(None, "cols", "rows"), check_vma=False
    )
```

```python
import functools

import jax
import jax.numpy as jnp
from jax import lax
from jax.experimental import pallas as pl
from jax.experimental.pallas import tpu as pltpu
from jax.sharding import PartitionSpec as P

LANES = 128
LEAF = 32
SUB = 16
CHUNK = 512
SELECT = 512
MICRO = 1 << 29
MIB = 1 << 20
ALMOST_ALL = 52 * MIB


def masks_of(size):
    return [1 << bit for bit in reversed(range(size.bit_length() - 1))]


def dot(left, right, left_dim=1, right_dim=0):
    return lax.dot_general(
        left, right, (((left_dim,), (right_dim,)), ((), ())), preferred_element_type=jnp.float32
    )


def split(x):
    high = x.astype(jnp.bfloat16)
    return high, (x - high.astype(jnp.float32)).astype(jnp.bfloat16)


def product_narrow(left, right, right_dim=0):
    rows = left.shape[0]
    both = dot(jnp.concatenate(split(left), 0), right, 1, right_dim)
    return both[:rows] + both[rows:]


def product_wide(left, right):
    left_high, left_low = split(left)
    right_high, right_low = split(right)
    return dot(
        jnp.concatenate([left_high, left_low, left_high], 1),
        jnp.concatenate([right_high, right_high, right_low], 0),
    )


def iota(shape, dim):
    return lax.broadcasted_iota(jnp.int32, shape, dim)


def as_column(row):
    size = row.shape[1]
    square = (size, size)
    return jnp.sum(
        jnp.where(iota(square, 0) == iota(square, 1), jnp.broadcast_to(row, square), 0.0),
        axis=1,
        keepdims=True,
    )


def pack(x):
    half = x.shape[0] // 2
    return jnp.concatenate([x[:half], x[half:]], 1)


def select_kernel(slot_count, pivots_ref, vectors_ref, integrals_ref, *refs):
    panels, block_cols, _ = integrals_ref.shape
    found_ref, out_refs = refs[0], refs[1 : 1 + panels]
    vec, ints, local_pivots, sems = refs[1 + panels :]
    part, row_count = vec.shape
    width = pivots_ref.shape[1]
    listed = pltpu.make_async_copy(pivots_ref, local_pivots, sems.at[sems.shape[0] - 1])
    listed.start()
    lanes = panels * slot_count
    first = pl.multiple_of(lax.axis_index("cols") * part, part)
    step = min(SELECT, row_count)
    count = row_count // step
    copies = []
    for n in range(count):
        at = pl.ds(n * step, step)
        copies.append(
            pltpu.make_async_copy(
                vectors_ref.at[pl.ds(first, part), at], vec.at[:, at], sems.at[n]
            )
        )
    whole = pltpu.make_async_copy(integrals_ref, ints, sems.at[count])
    for copy in copies[:1] + [whole] + copies[1:]:
        copy.start()
    listed.wait()
    start = (lax.axis_index("rows") * row_count).astype(jnp.float32)
    square = (width, width)
    target = jnp.zeros((1, lanes), jnp.float32)
    for panel in range(panels):
        local = local_pivots[panel : panel + 1, :].astype(jnp.float32) - start
        mine = ((local >= 0.0) & (local < row_count)).astype(jnp.float32)
        earlier = iota(square, 1) < iota(square, 0)
        rank = jnp.sum(
            jnp.where(earlier, jnp.broadcast_to(mine, square), 0.0), axis=1, keepdims=True
        )
        held = as_column(jnp.where(mine > 0.0, local + 1.0, 0.0))
        slot = iota((width, lanes), 1).astype(jnp.float32) - panel * slot_count
        target = target + jnp.sum(jnp.where(rank == slot, held, 0.0), axis=0, keepdims=True)
    target = target.astype(jnp.int32) - 1
    whole.wait()
    outs = [
        pltpu.make_async_copy(ints.at[panel], out_refs[panel], sems.at[count + 1 + panel])
        for panel in range(panels)
    ]
    for copy in outs:
        copy.start()
    found = jnp.zeros((part + panels * block_cols, lanes), jnp.float32)
    for n, copy in enumerate(copies):
        copy.wait()
        at = slice(n * step, (n + 1) * step)
        pick = jnp.where(iota((step, lanes), 0) + n * step == target, 1.0, 0.0).astype(jnp.bfloat16)
        left = jnp.concatenate([vec[:, at]] + [ints[panel, :, at] for panel in range(panels)], 0)
        found = found + dot(left, pick)
    common = part + block_cols
    found_ref[:common, :] = found[:common].astype(jnp.bfloat16)
    found_ref[common:, :] = pack(found[common:, slot_count:]).astype(jnp.bfloat16)
    for copy in outs:
        copy.wait()


def select(pivots, vectors, integrals, slot_count, part):
    panels, block_cols, row_count = integrals.shape
    rows = part + block_cols + block_cols // 2
    outs = [jax.ShapeDtypeStruct((rows, panels * slot_count), jnp.bfloat16)]
    outs += [jax.ShapeDtypeStruct((block_cols, row_count), jnp.bfloat16)] * panels
    results = pl.pallas_call(
        functools.partial(select_kernel, slot_count),
        out_shape=outs,
        in_specs=[pl.BlockSpec(memory_space=pl.ANY)] * 3,
        out_specs=[pl.BlockSpec(memory_space=pltpu.VMEM)]
        + [pl.BlockSpec(memory_space=pltpu.HBM)] * panels,
        scratch_shapes=[
            pltpu.VMEM((part, row_count), jnp.bfloat16),
            pltpu.VMEM(integrals.shape, jnp.bfloat16),
            pltpu.VMEM(pivots.shape, jnp.int32),
            pltpu.SemaphoreType.DMA((row_count // min(SELECT, row_count) + 2 + panels,)),
        ],
        compiler_params=pltpu.CompilerParams(vmem_limit_bytes=ALMOST_ALL),
        cost_estimate=pl.CostEstimate(flops=MICRO * 2, bytes_accessed=3 * MIB, transcendentals=0),
        name="select",
    )(pivots, vectors, integrals)
    return results[0], results[1:]


def places_kernel(weights, slot_count, row_count, pivots_ref, out_ref):
    panels, width = pivots_ref.shape
    lanes = panels * slot_count
    shift = row_count.bit_length() - 1
    me = lax.axis_index("rows")
    square = (width, width)
    places = []
    for panel in range(panels):
        owner = lax.shift_right_logical(
            pivots_ref[panel : panel + 1, :], jnp.full((1, width), shift, jnp.int32)
        )
        floats = owner.astype(jnp.float32)
        same = jnp.broadcast_to(floats, square) == as_column(floats)
        earlier = iota(square, 0) < iota(square, 1)
        rank = jnp.sum(
            jnp.where(same & earlier, 1.0, 0.0), axis=0, keepdims=True
        ).astype(jnp.int32)
        apart = owner ^ me
        block = jnp.zeros_like(owner)
        for mask, weight in weights:
            block = block + jnp.where((apart & mask) != 0, weight, 0)
        places.append(block * lanes + rank)
    out_ref[0:1, :] = jnp.concatenate([places[0], places[1] + slot_count], 1)
    out_ref[1:2, :] = jnp.concatenate([places[1], places[1] + slot_count], 1)


def places_of(pivots, weights, slot_count, row_count):
    return pl.pallas_call(
        functools.partial(places_kernel, weights, slot_count, row_count),
        out_shape=jax.ShapeDtypeStruct((2, 2 * pivots.shape[1]), jnp.int32),
        in_specs=[pl.BlockSpec(memory_space=pltpu.VMEM)],
        out_specs=pl.BlockSpec(memory_space=pltpu.VMEM),
        compiler_params=pltpu.CompilerParams(vmem_limit_bytes=16 * MIB),
        cost_estimate=pl.CostEstimate(flops=MICRO, bytes_accessed=MIB, transcendentals=0),
        name="places",
    )(pivots)


def compact_kernel(places_ref, *refs):
    pieces, outs = refs[:-2], refs[-2:]
    depth, rows, lanes = pieces[0].shape
    common, width = outs[0].shape
    both, halves = places_ref[0:1, :], places_ref[1:2, :]
    main = jnp.zeros((common, 2 * width), jnp.float32)
    rest = jnp.zeros((rows - common, 2 * width), jnp.float32)
    for i in range(len(pieces) * depth):
        lane = iota((lanes, 2 * width), 0) + i * lanes
        x = pieces[i // depth][i % depth]
        main = main + dot(x[:common], jnp.where(lane == both, 1.0, 0.0).astype(jnp.bfloat16))
        rest = rest + dot(x[common:], jnp.where(lane == halves, 1.0, 0.0).astype(jnp.bfloat16))
    outs[0][...] = main[:, :width].astype(jnp.bfloat16)
    outs[1][:common, :] = main[:, width:].astype(jnp.bfloat16)
    outs[1][common:rows, :] = rest[:, :width].astype(jnp.bfloat16)
    outs[1][rows:, :] = rest[:, width:].astype(jnp.bfloat16)


def compact(places, pieces, part):
    rows = pieces[0].shape[1]
    width = places.shape[1] // 2
    block_cols = (rows - part) * 2 // 3
    return pl.pallas_call(
        compact_kernel,
        out_shape=[
            jax.ShapeDtypeStruct((part + block_cols, width), jnp.bfloat16),
            jax.ShapeDtypeStruct((part + 2 * block_cols, width), jnp.bfloat16),
        ],
        in_specs=[pl.BlockSpec(memory_space=pltpu.VMEM)] * (1 + len(pieces)),
        out_specs=[pl.BlockSpec(memory_space=pltpu.VMEM)] * 2,
        compiler_params=pltpu.CompilerParams(vmem_limit_bytes=16 * MIB),
        cost_estimate=pl.CostEstimate(flops=MICRO, bytes_accessed=MIB, transcendentals=0),
        name="compact",
    )(places, *pieces)


def eliminate(block, columns, offset):
    vregs = LEAF // 8
    tiles = {g: [x[8 * v : 8 * v + 8] for v in range(vregs)] for g, x in block.items()}
    sublane = iota((8, LANES), 0)
    pivots = [jnp.zeros((8, LANES), jnp.float32) for _ in range(vregs)]
    for sub in range(0, LEAF, SUB):
        first = sub // 8
        diagonal = tiles[columns][first:]
        cols = [
            [
                jnp.broadcast_to(x[:, offset + sub + k : offset + sub + k + 1], (8, LANES))
                for x in diagonal
            ]
            for k in range(SUB)
        ]
        for j in range(SUB):
            jv, jr = j // 8, j % 8
            live = range(jv, len(diagonal))
            pivot = jnp.broadcast_to(cols[j][jv][jr : jr + 1, :], (8, LANES))
            inverse = 1.0 / pivot
            factor = {v: cols[j][v] * inverse for v in live}
            factor[jv] = jnp.where(sublane > jr, factor[jv], 0.0)
            pivots[first + jv] = jnp.where(sublane == jr, pivot, pivots[first + jv])
            for k in range(j + 1, SUB):
                entry = jnp.broadcast_to(cols[j][k // 8][k % 8 : k % 8 + 1, :], (8, LANES))
                for v in range(k // 8, len(diagonal)):
                    cols[k][v] = cols[k][v] - factor[v] * entry
            for rows in tiles.values():
                entry = jnp.broadcast_to(rows[first + jv][jr : jr + 1, :], (8, LANES))
                for v in live:
                    rows[first + v] = rows[first + v] - factor[v] * entry
    scale = [lax.rsqrt(pivot) for pivot in pivots]
    return {
        g: jnp.concatenate([x * y for x, y in zip(rows, scale)], 0) for g, rows in tiles.items()
    }


def start_factor(matrix, work):
    width = matrix.shape[0]
    square = (width, width)
    work[:, :width] = 0.5 * (matrix + matrix.T)
    work[:, width:] = jnp.where(iota(square, 0) == iota(square, 1), 1.0, 0.0)


def lanes_of(g):
    return slice(g * LANES, (g + 1) * LANES)


def run_leaves(work, begin, end):
    width = work.shape[0]
    half = width // LANES
    block = None
    for start in range(begin, end, LEAF):
        following = start + LEAF
        rights = [half + g for g in range((following - 1) // LANES + 1)]
        groups = list(range(start // LANES, half)) + rights
        if block is None:
            block = {g: work[start:following, lanes_of(g)] for g in groups}
        upper = eliminate(block, start // LANES, start % LANES)
        for g in rights:
            work[start:following, lanes_of(g)] = upper[g]
        if following == width:
            break
        lefts = list(range(following // LANES, half))
        used = lefts + rights
        base = lefts[0] * LANES
        high, low = split(jnp.concatenate([upper[g] for g in used], 1))
        right = jnp.concatenate([high, high, low], 0)

        def product(first, last):
            a = high[:, first - base : last - base]
            b = low[:, first - base : last - base]
            return dot(jnp.concatenate([a, b, a], 0), right, 0, 0)

        stop = following + LEAF
        change = product(following, stop)
        block = {}
        for g in lefts + [half + g for g in range((stop - 1) // LANES + 1)]:
            block[g] = work[following:stop, lanes_of(g)]
            if g in used:
                block[g] = block[g] - change[:, lanes_of(used.index(g))]
        if following == end:
            for g, x in block.items():
                work[following:stop, lanes_of(g)] = x
        if stop < width:
            change = product(stop, width)
            for i, g in enumerate(used):
                work[stop:, lanes_of(g)] = work[stop:, lanes_of(g)] - change[:, lanes_of(i)]


def first_kernel(apart, part, *refs):
    count = len(apart)
    picked = refs[:count]
    work, rows_of, ints = refs[count:]
    me = lax.axis_index("cols")
    block_cols = picked[0].shape[0] - part
    for ref, bits in zip(picked, apart):
        at = pl.multiple_of((me ^ bits) * block_cols, block_cols)
        rows_of[pl.ds(pl.multiple_of((me ^ bits) * part, part), part), :] = ref[:part, :]
        ints[pl.ds(at, block_cols), :] = ref[part:, :].astype(jnp.float32)
    at_pivots = rows_of[...]
    start_factor(ints[...] - dot(at_pivots, at_pivots, 0, 0), work)
    run_leaves(work, 0, work.shape[0] // 2)


def first_half(picked, apart, part):
    count = len(apart)
    _, width = picked[0].shape
    return pl.pallas_call(
        functools.partial(first_kernel, apart, part),
        out_shape=jax.ShapeDtypeStruct((width, 2 * width), jnp.float32),
        in_specs=[pl.BlockSpec(memory_space=pltpu.VMEM)] * count,
        out_specs=pl.BlockSpec(memory_space=pltpu.VMEM),
        scratch_shapes=[
            pltpu.VMEM((count * part, width), jnp.bfloat16),
            pltpu.VMEM((width, width), jnp.float32),
        ],
        compiler_params=pltpu.CompilerParams(vmem_limit_bytes=16 * MIB),
        cost_estimate=pl.CostEstimate(flops=4 * MICRO, bytes_accessed=MIB, transcendentals=0),
        name="first_half",
    )(*picked)


def second_kernel(before_ref, work):
    work[...] = before_ref[...]
    run_leaves(work, work.shape[0] // 2, work.shape[0])


def second_half(work):
    return pl.pallas_call(
        second_kernel,
        out_shape=jax.ShapeDtypeStruct(work.shape, work.dtype),
        in_specs=[pl.BlockSpec(memory_space=pltpu.VMEM)],
        out_specs=pl.BlockSpec(memory_space=pltpu.VMEM),
        compiler_params=pltpu.CompilerParams(vmem_limit_bytes=16 * MIB),
        cost_estimate=pl.CostEstimate(flops=4 * MICRO, bytes_accessed=MIB, transcendentals=0),
        name="second_half",
    )(work)


def third_kernel(apart, part, *refs):
    count = len(apart)
    work0, picked0, picked1 = refs[0], refs[1 : 1 + count], refs[1 + count : 1 + 2 * count]
    work1, rows_of, ahead_ref, ints0, ints1 = refs[1 + 2 * count :]
    me = lax.axis_index("cols")
    width = work0.shape[0]
    block_cols = picked0[0].shape[0] - part
    for i, bits in enumerate(apart):
        at = pl.ds(pl.multiple_of((me ^ bits) * part, part), part)
        rows_of[at, :width] = picked0[i][:part, :]
        rows_of[at, width:] = picked1[i][:part, :]
        at = pl.ds(pl.multiple_of((me ^ bits) * block_cols, block_cols), block_cols)
        ints0[at, :] = picked1[i][part : part + block_cols, :].astype(jnp.float32)
        ints1[at, :] = picked1[i][part + block_cols :, :].astype(jnp.float32)
    gram = dot(rows_of[...], rows_of[:, width:], 0, 0)
    ahead = product_wide(work0[:, width:], ints0[...] - gram[:width]).astype(jnp.bfloat16)
    ahead_ref[...] = ahead
    start_factor(ints1[...] - gram[width:] - dot(ahead, ahead, 0, 0), work1)
    run_leaves(work1, 0, width // 2)


def third_half(work0, picked0, picked1, apart, part):
    count = len(apart)
    width = work0.shape[0]
    return pl.pallas_call(
        functools.partial(third_kernel, apart, part),
        out_shape=[
            jax.ShapeDtypeStruct(work0.shape, jnp.float32),
            jax.ShapeDtypeStruct((count * part, 2 * width), jnp.bfloat16),
            jax.ShapeDtypeStruct((width, width), jnp.bfloat16),
        ],
        in_specs=[pl.BlockSpec(memory_space=pltpu.VMEM)] * (1 + 2 * count),
        out_specs=[pl.BlockSpec(memory_space=pltpu.VMEM)] * 3,
        scratch_shapes=[pltpu.VMEM((width, width), jnp.float32)] * 2,
        compiler_params=pltpu.CompilerParams(vmem_limit_bytes=16 * MIB),
        cost_estimate=pl.CostEstimate(flops=5 * MICRO, bytes_accessed=MIB, transcendentals=0),
        name="third_half",
    )(work0, *picked0, *picked1)


def fourth_kernel(apart, block_cols, work0, before_ref, rows_of, ahead, left, work1):
    width = work0.shape[0]
    square = (width, width)
    me = lax.axis_index("cols")
    mine = pl.ds(pl.multiple_of(me * block_cols, block_cols), block_cols)
    work1[...] = before_ref[...]
    lane = iota(square, 1)
    source = iota(square, 0)
    arrive = jnp.zeros(square, jnp.float32)
    for i, bits in enumerate(apart):
        shifted = lane + ((me ^ bits) - i) * block_cols
        here = (lane >= i * block_cols) & (lane < (i + 1) * block_cols)
        arrive = jnp.where(here & (source == shifted), 1.0, arrive)
    arrive = arrive.astype(jnp.bfloat16)
    same = jnp.where(source == lane, 1.0, 0.0).astype(jnp.bfloat16)
    inverse_high, inverse_low = split(work0[:, width:])
    through = dot(ahead[...], inverse_high, 0, 0) + dot(ahead[...], inverse_low, 0, 0)
    through_high, through_low = split(through)
    early, late = rows_of[:, :width], rows_of[:, width:]
    on_vectors = dot(
        jnp.concatenate([same, -through_high, -through_low], 1),
        jnp.concatenate([late, early, early], 1),
        1,
        1,
    )
    right_high, right_low = split(
        jnp.concatenate([-product_narrow(through, arrive), -on_vectors], 1)
    )
    right_high = jnp.concatenate([right_high[:, :width], arrive, right_high[:, width:]], 1)
    right_low = jnp.concatenate(
        [right_low[:, :width], jnp.zeros_like(arrive), right_low[:, width:]], 1
    )
    right = jnp.concatenate([right_high, right_high, right_low], 0)
    inverse0 = work0[mine, width:]
    top = jnp.concatenate(
        [
            product_narrow(inverse0, arrive),
            jnp.zeros((block_cols, width), jnp.float32),
            -product_narrow(inverse0, early, 1),
        ],
        1,
    )
    top_high, top_low = split(top)
    left[:block_cols, :] = top_high
    left[2 * block_cols : 3 * block_cols, :] = top_low

    run_leaves(work1, width // 2, width)
    high, low = split(work1[mine, width:])
    low_high, low_low = split(dot(jnp.concatenate([high, low, high], 1), right))
    left[block_cols : 2 * block_cols, :] = low_high
    left[3 * block_cols :, :] = low_low


def fourth_half(work0, work1, rows_of, ahead, apart, block_cols):
    width = work0.shape[0]
    return pl.pallas_call(
        functools.partial(fourth_kernel, apart, block_cols),
        out_shape=jax.ShapeDtypeStruct(
            (4 * block_cols, 2 * width + rows_of.shape[0]), jnp.bfloat16
        ),
        in_specs=[pl.BlockSpec(memory_space=pltpu.VMEM)] * 4,
        out_specs=pl.BlockSpec(memory_space=pltpu.VMEM),
        scratch_shapes=[pltpu.VMEM(work0.shape, jnp.float32)],
        compiler_params=pltpu.CompilerParams(vmem_limit_bytes=16 * MIB),
        cost_estimate=pl.CostEstimate(flops=5 * MICRO, bytes_accessed=MIB, transcendentals=0),
        name="fourth_half",
    )(work0, work1, rows_of, ahead)


def finish_kernel(left, vectors_ref, *refs):
    blocks, (out_ref, result, out_sems) = refs[:-3], refs[-3:]
    pairs = vectors_ref.shape[1]
    block_cols = blocks[0].shape[0]
    both = len(blocks) * block_cols
    second = jnp.concatenate(
        [
            left[block_cols : 2 * block_cols, both // 2 : both],
            left[3 * block_cols :, both // 2 : both],
        ],
        0,
    )
    outs = []
    for n in range(pairs // CHUNK):
        at = slice(n * CHUNK, (n + 1) * CHUNK)
        right0, right1 = (
            jnp.concatenate([ref[:, at] for ref in some], 0)
            for some in (blocks[: len(blocks) // 2], blocks[len(blocks) // 2 :])
        )
        halves = dot(left[:, both:], vectors_ref[:, at]) + dot(left[:, : both // 2], right0)
        value = halves[: 2 * block_cols] + halves[2 * block_cols :]
        halves = dot(second, right1)
        last = value[block_cols:] + (halves[:block_cols] + halves[block_cols:])
        result[0, :, at] = value[:block_cols]
        result[1, :, at] = last
        outs.append(
            pltpu.make_async_copy(result.at[:, :, at], out_ref.at[:, :, at], out_sems.at[n])
        )
        outs[-1].start()
    for copy in outs:
        copy.wait()


def finish(left, vectors, blocks):
    block_cols, pairs = blocks[0].shape
    return pl.pallas_call(
        finish_kernel,
        out_shape=jax.ShapeDtypeStruct((2, block_cols, pairs), jnp.float32),
        in_specs=[pl.BlockSpec(memory_space=pltpu.VMEM)] * (2 + len(blocks)),
        out_specs=pl.BlockSpec(memory_space=pl.ANY),
        scratch_shapes=[
            pltpu.VMEM((2, block_cols, pairs), jnp.float32),
            pltpu.SemaphoreType.DMA((pairs // CHUNK,)),
        ],
        compiler_params=pltpu.CompilerParams(vmem_limit_bytes=24 * MIB),
        cost_estimate=pl.CostEstimate(
            flops=6 * MICRO, bytes_accessed=16 * MIB, transcendentals=0
        ),
        name="finish",
    )(left, vectors, *blocks)


def per_device(vectors, integrals, pivots):
    prior, row_count = vectors.shape
    _, width = pivots.shape
    owners, col_count = lax.axis_size("rows"), lax.axis_size("cols")
    block_cols = integrals.shape[1]
    slot_count = 2 * width // owners
    part = prior // col_count

    def swap(x, axis, mask):
        size = lax.axis_size(axis)
        return lax.ppermute(x, axis, [(i, i ^ mask) for i in range(size)])

    def near(pieces):
        return [swap(piece, "cols", near_mask) for piece in pieces]

    far_mask, near_mask = masks_of(col_count)
    apart = [0, far_mask, near_mask, far_mask ^ near_mask]

    found, ints = select(pivots, vectors, integrals, slot_count, part)
    masks = masks_of(owners)
    held = found[None]
    depth, weights = 1, []
    for mask in masks[:-3]:
        held = jnp.concatenate([held, swap(held, "rows", mask)], 0)
        weights.append((mask, depth))
        depth = 2 * depth
    weights += [(mask, depth << i) for i, mask in enumerate(masks[-3:])]
    passed = swap(held, "rows", masks[-3])
    pieces = [held, passed]
    for mask in (masks[-2], masks[-1], masks[-2] ^ masks[-1]):
        pieces.append(swap(held, "rows", mask))
        pieces.append(swap(passed, "rows", mask))
    places = places_of(pivots, weights, slot_count, row_count)
    own0, own1 = compact(places, pieces, part)

    far0 = swap(ints[0], "cols", far_mask)
    other0 = swap(own0, "cols", far_mask)
    other1 = swap(own1, "cols", far_mask)
    picked0 = [own0, other0] + near([own0]) + near([other0])
    beside1 = near([own1])
    beside = near(ints)
    far1 = swap(ints[1], "cols", far_mask)
    work0 = first_half(picked0, apart, part)
    work0, other1 = lax.optimization_barrier((work0, other1))
    picked1 = [own1, other1] + beside1 + near([other1])
    blocks = [ints[0], far0, beside[0]] + near([far0])
    work0 = second_half(work0)
    work1, rows_of, ahead = third_half(work0, picked0, picked1, apart, part)
    work1, far1 = lax.optimization_barrier((work1, far1))
    blocks += [ints[1], far1, beside[1]] + near([far1])
    left = fourth_half(work0, work1, rows_of, ahead, apart, block_cols)
    return finish(left, vectors, blocks)


def solution(mesh):
    placed = (P(None, "rows"), P(None, "cols", "rows"), P())

    return jax.shard_map(
        per_device, mesh=mesh, in_specs=placed, out_specs=P(None, "cols", "rows"), check_vma=False
    )
```
